32 devices in a mesh: seq: 8 (over z, core), batch: 4 (over y, x).
Axes of the slice: x: 2, y: 2, z: 4, core: 2. Of those that a mesh axis runs over, the one named last changes fastest.
Arguments:
- tokens: bfloat16 [4, 2048, 1152], P('batch', 'seq'), may hold values from -6 to 6
- long_skip: bfloat16 [4, 2048, 1152], P('batch', 'seq'), may hold values from -6 to 6
- lengths: int32 [4, 4], P('batch'), may hold values from 0 to 1026, as said below
- skip_weight: bfloat16 [2304, 1152], replicated, may hold values from -0.125 to 0.125
- skip_bias: bfloat16 [1152], replicated, may hold values from -3 to 3
- attention_gain: bfloat16 [1152], replicated, may hold values from 0.099609375 to 1.8984375
- attention_shift: bfloat16 [1152], replicated, may hold values from -3 to 3
- qkv_weight: bfloat16 [1152, 3456], replicated, may hold values from -0.1875 to 0.1875
- out_weight: bfloat16 [1152, 1152], replicated, may hold values from -2 to 2
- out_bias: bfloat16 [1152], replicated, may hold values from -3 to 3
- mlp_gain: bfloat16 [1152], replicated, may hold values from 0.099609375 to 1.8984375
- mlp_shift: bfloat16 [1152], replicated, may hold values from -3 to 3
- hidden_weight: bfloat16 [1152, 4608], replicated, may hold values from -0.1875 to 0.1875
- hidden_bias: bfloat16 [4608], replicated, may hold values from -3 to 3
- down_weight: bfloat16 [4608, 1152], replicated, may hold values from -0.09375 to 0.09375
- down_bias: bfloat16 [1152], replicated, may hold values from -3 to 3
- cotangent: bfloat16 [4, 2048, 1152], P('batch', 'seq'), may hold values from -6 to 6
Outputs:
- output: bfloat16 [4, 2048, 1152], P('batch', 'seq')
- grad_tokens: float32 [4, 2048, 1152], P('batch', 'seq')
- grad_long_skip: float32 [4, 2048, 1152], P('batch', 'seq')
- grad_skip_weight: float32 [2304, 1152], P('batch', 'seq')
- grad_skip_bias: float32 [1152], replicated
- grad_attention_gain: float32 [1152], replicated
- grad_attention_shift: float32 [1152], replicated
- grad_qkv_weight: float32 [1152, 3456], P('batch', 'seq')
- grad_out_weight: float32 [1152, 1152], P('batch', 'seq')
- grad_out_bias: float32 [1152], replicated
- grad_mlp_gain: float32 [1152], replicated
- grad_mlp_shift: float32 [1152], replicated
- grad_hidden_weight: float32 [1152, 4608], P('batch', 'seq')
- grad_hidden_bias: float32 [4608], replicated
- grad_down_weight: float32 [4608, 1152], P('batch', 'seq')
- grad_down_bias: float32 [1152], replicated
The draws below stay inside these ranges and needn't reach their ends.
Inputs may be any that keep to these rules, and one draw needn't show every extreme that they name: Row g lists the lengths of group g's items in the order in which they lie along the group's 2048 positions. Each entry is 258, 1026 or 0, every row has one or more entries 1026, zeros stand only after the last nonzero entry, and the row's total leaves fewer than 258 positions of padding at the end.
All inputs are finite; a program needn't handle non-finite values.
Results may differ from the reference program's by a relative error of at most 0.013.
Values may be sent and summed in bfloat16 or wider, within the bound.
A program may use at most 256 MiB of HBM per device.

```python
import math
from functools import partial
import jax
import jax.numpy as jnp
from jax import lax

D = 1152
HEADS = 16
HD = 72
FF = 4608
SHORT = 258
LONG = 1026
GROUP_LEN = 2048
GROUPS = 4
ITEMS = 4


def draw_lengths(key, part):
    most_long = GROUP_LEN // LONG

    def one_group(subkey):
        key_count, key_order = jax.random.split(subkey)
        longs = jax.random.randint(key_count, (), 1, most_long + 1)
        shorts = (GROUP_LEN - longs * LONG) // SHORT
        slots = jnp.arange(ITEMS, dtype=jnp.int32)
        kinds = jnp.where(slots < longs, LONG, jnp.where(slots < longs + shorts, SHORT, 0)).astype(jnp.int32)
        ranks = jax.random.randint(key_order, (ITEMS,), 0, 1 << 20) * ITEMS + slots
        ranks = jnp.where(slots < longs + shorts, ranks, (1 << 30) + slots)
        order = jnp.argsort(ranks)
        return kinds[order].astype(jnp.int32)
    return jax.vmap(one_group)(jax.random.split(key, GROUPS))


def steps_of(rng, extent, shards, least, largest):
    level = 1.0
    for position, blocks in shards:
        heights = jax.random.uniform(jax.random.fold_in(jax.random.fold_in(rng, 6), position), (blocks,), jnp.float32, least / len(shards), largest / len(shards))
        level = level * jnp.repeat(jnp.exp(heights), extent[position] // blocks).reshape((-1,) + (1,) * (len(extent) - 1 - position))
    return level


def bell_draw(rng, extent, deviation, most, cuts=(), held_as=jnp.bfloat16):
    drawn = jax.random.normal(rng, extent, jnp.float32) * deviation
    if len(cuts) > 0:
        drawn = steps_of(rng, extent, cuts, -0.22, 0.18) * drawn
    return jnp.clip(drawn, min=-most, max=most).astype(held_as)


def setup_inputs(seed: int = 0) -> dict:
    key_of = jax.random.split(jax.random.key(seed), 18)
    tokens = bell_draw(key_of[0], (GROUPS, GROUP_LEN, D), 1.0, 6.0, ((0, 4), (1, 8)))
    long_skip = bell_draw(key_of[1], (GROUPS, GROUP_LEN, D), 1.0, 6.0, ((0, 4), (1, 8)))
    lengths = draw_lengths(jax.random.fold_in(key_of[17], 71), 0)
    skip_weight = bell_draw(key_of[3], (2 * D, D), (2 * D) ** -0.5, 0.125)
    skip_bias = bell_draw(key_of[4], (D,), 0.5, 3.0)
    attention_gain = jnp.clip(1.0 + 0.18 * jax.random.normal(key_of[5], (D,), jnp.float32), 0.099609375, 1.8984375).astype(jnp.bfloat16)
    attention_shift = bell_draw(key_of[6], (D,), 0.5, 3.0)
    qkv_weight = bell_draw(key_of[7], (D, 3 * D), D ** -0.5, 0.1875)
    out_weight = bell_draw(key_of[8], (D, D), (max(D // 128, 2)) ** -0.5, 2.0)
    out_bias = bell_draw(key_of[9], (D,), 0.5, 3.0)
    mlp_gain = jnp.clip(1.0 + 0.18 * jax.random.normal(key_of[10], (D,), jnp.float32), 0.099609375, 1.8984375).astype(jnp.bfloat16)
    mlp_shift = bell_draw(key_of[11], (D,), 0.5, 3.0)
    hidden_weight = bell_draw(key_of[12], (D, FF), D ** -0.5, 0.1875)
    hidden_bias = bell_draw(key_of[13], (FF,), 0.5, 3.0)
    down_weight = bell_draw(key_of[14], (FF, D), FF ** -0.5, 0.09375)
    down_bias = bell_draw(key_of[15], (D,), 0.5, 3.0)
    cotangent = bell_draw(key_of[16], (GROUPS, GROUP_LEN, D), 1.0, 6.0, ((0, 4), (1, 8)))
    return {"tokens": tokens, "long_skip": long_skip, "lengths": lengths, "skip_weight": skip_weight, "skip_bias": skip_bias, "attention_gain": attention_gain, "attention_shift": attention_shift, "qkv_weight": qkv_weight, "out_weight": out_weight, "out_bias": out_bias, "mlp_gain": mlp_gain, "mlp_shift": mlp_shift, "hidden_weight": hidden_weight, "hidden_bias": hidden_bias, "down_weight": down_weight, "down_bias": down_bias, "cotangent": cotangent}


@jax.custom_vjp
def low(v):
    return lax.optimization_barrier(v.astype(jnp.bfloat16)).astype(jnp.float32)

@jax.custom_vjp
def low_back(v):
    return v

def low_keep(v):
    return (low(v), None)

def low_pass(kept, grad):
    return (grad,)

def back_keep(v):
    return (v, None)

def back_low(kept, grad):
    return (low(grad),)
low.defvjp(low_keep, low_pass)
low_back.defvjp(back_keep, back_low)
norm_eps = 1e-05

def matmul(left, right):
    return jnp.dot(left, right, precision=lax.Precision.HIGHEST, preferred_element_type=jnp.float32)

def layer_norm(inputs, gain, shift):
    mean_row = lax.optimization_barrier(jnp.mean(inputs, axis=-1, keepdims=True))
    centred = inputs - mean_row
    spread = lax.optimization_barrier(jnp.mean(centred * centred, axis=-1, keepdims=True))
    return centred * lax.rsqrt(spread + norm_eps) * gain + shift

def exact_gelu(inputs):
    return jax.nn.gelu(inputs, approximate=False)

def segments(row_lengths, group_len):
    ends = jnp.cumsum(row_lengths.astype(jnp.int32)).astype(jnp.int32)
    places = jnp.arange(group_len, dtype=jnp.int32)
    return lax.optimization_barrier(jnp.sum((places[:, None] >= ends[None, :]).astype(jnp.int32), axis=1)).astype(jnp.int32)

def attend_group(pieces):
    query_group, key_group, value_group, segment = pieces
    length = query_group.shape[0]
    block_rows = min(512, length)
    block_count = length // block_rows
    key_heads = key_group.reshape(length, HEADS, HD)
    value_heads = value_group.reshape(length, HEADS, HD)
    score_scale = 1.0 / math.sqrt(HD)

    def one_block(parts):
        query_block, seg_block = parts
        raw = jnp.einsum('bhd,khd->hbk', query_block, key_heads, precision=lax.Precision.HIGHEST)
        scores = low_back(raw * score_scale)
        allowed = (seg_block[:, None] == segment[None, :])[None]
        scores = jnp.where(allowed, scores, -jnp.inf)
        log_total = jax.nn.logsumexp(scores, axis=2, keepdims=True)
        probs = low(jnp.exp(scores - log_total))
        context = jnp.einsum('hbk,khd->bhd', probs, value_heads, precision=lax.Precision.HIGHEST)
        return context.reshape(block_rows, HEADS * HD)
    result = lax.map(jax.checkpoint(one_block), (query_group.reshape(block_count, block_rows, HEADS, HD), segment.reshape(block_count, block_rows)))
    return result.reshape(length, HEADS * HD)

def forward(tokens, long_skip, skip_weight, skip_bias, attention_gain, attention_shift, qkv_weight, out_weight, out_bias, mlp_gain, mlp_shift, hidden_weight, hidden_bias, down_weight, down_bias, segment):
    groups, length, width = tokens.shape
    joined = jnp.concatenate([tokens, long_skip], axis=2).reshape(groups * length, 2 * width)
    mixed = low_back(matmul(joined, skip_weight) + skip_bias)
    normed_one = low(layer_norm(mixed, attention_gain, attention_shift))
    packed = low(low_back(matmul(normed_one, qkv_weight)))
    query_all = packed[:, :width].reshape(groups, length, width)
    key_all = packed[:, width:2 * width].reshape(groups, length, width)
    value_all = packed[:, 2 * width:].reshape(groups, length, width)
    context = lax.map(attend_group, (query_all, key_all, value_all, segment))
    context = low(low_back(context.reshape(groups * length, width)))
    attended = low_back(matmul(context, out_weight) + out_bias)
    middle = mixed + attended
    normed_two = low(layer_norm(middle, mlp_gain, mlp_shift))
    hidden_pre = low_back(matmul(normed_two, hidden_weight) + hidden_bias)
    hidden_act = low(exact_gelu(hidden_pre))
    result = middle + matmul(hidden_act, down_weight) + down_bias
    return result.reshape(groups, length, width)

def reference(tokens, long_skip, lengths, skip_weight, skip_bias, attention_gain, attention_shift, qkv_weight, out_weight, out_bias, mlp_gain, mlp_shift, hidden_weight, hidden_bias, down_weight, down_bias, cotangent):
    segment = jax.vmap(partial(segments, group_len=GROUP_LEN))(lengths)
    floats = [array.astype(jnp.float32) for array in (tokens, long_skip, skip_weight, skip_bias, attention_gain, attention_shift, qkv_weight, out_weight, out_bias, mlp_gain, mlp_shift, hidden_weight, hidden_bias, down_weight, down_bias)]

    def layer(*params):
        return forward(*params, segment)
    output, pullback = jax.vjp(layer, *floats)
    grads = pullback(cotangent.astype(jnp.float32))
    return (output.astype(jnp.bfloat16), grads[0], grads[1], grads[2], grads[3], grads[4], grads[5], grads[6], grads[7], grads[8], grads[9], grads[10], grads[11], grads[12], grads[13], grads[14])
```

```python
import math

import jax
import jax.numpy as jnp
from jax import lax
from jax.sharding import PartitionSpec as P

HD = 72


norm_eps = 1e-05


def product(left, right):
    return jnp.dot(left, right, preferred_element_type=jnp.float32)


def contract_rows(left, right):
    return lax.dot_general(
        left, right, (((0,), (0,)), ((), ())), preferred_element_type=jnp.float32
    )


def times_transposed(left, right):
    return lax.dot_general(
        left, right, (((1,), (1,)), ((), ())), preferred_element_type=jnp.float32
    )


def column_sums(values):
    return jnp.sum(values.astype(jnp.float32), axis=0)


def layer_norm(inputs, gain, shift):
    mean_row = jnp.mean(inputs, axis=-1, keepdims=True)
    centred = inputs - mean_row
    spread = jnp.mean(centred * centred, axis=-1, keepdims=True)
    return centred * lax.rsqrt(spread + norm_eps) * gain + shift


def exact_gelu(inputs):
    return jax.nn.gelu(inputs, approximate=False)


def segments(row_lengths, group_len):
    ends = jnp.cumsum(row_lengths)
    places = jnp.arange(group_len, dtype=jnp.int32)
    return jnp.sum((places[:, None] >= ends[None, :]).astype(jnp.int32), axis=1)


def score_block(query_block, key_heads, seg_block, segment):
    raw = jnp.einsum("bhd,khd->hbk", query_block, key_heads, preferred_element_type=jnp.float32)
    scores = raw * (1.0 / math.sqrt(HD))
    allowed = (seg_block[:, None] == segment[None, :])[None]
    return jnp.where(allowed, scores, -jnp.inf)


def attend_forward(query_heads, key_flat, value_flat, segment):
    length, head_cols = query_heads.shape
    head_count = head_cols // HD
    block_rows = min(512, length)
    block_count = length // block_rows
    key_heads = key_flat.reshape(length, head_count, HD)
    value_heads = value_flat.reshape(length, head_count, HD)

    def one_block(pieces):
        query_block, seg_block = pieces
        scores = score_block(query_block, key_heads, seg_block, segment)
        row_max = jnp.max(scores, axis=2, keepdims=True)
        log_total = row_max + jnp.log(jnp.sum(jnp.exp(scores - row_max), axis=2, keepdims=True))
        probs_low = jnp.exp(scores - log_total).astype(jnp.bfloat16)
        context = jnp.einsum(
            "hbk,khd->bhd", probs_low, value_heads, preferred_element_type=jnp.float32
        )
        return (context.astype(jnp.bfloat16).reshape(block_rows, head_cols), log_total)

    context, log_total = lax.map(
        one_block,
        (
            query_heads.reshape(block_count, block_rows, head_count, HD),
            segment.reshape(block_count, block_rows),
        ),
    )
    return (context.reshape(length, head_cols), log_total)


def attend_backward(query_heads, key_flat, value_flat, segment, grad_context, log_total):
    length, head_cols = query_heads.shape
    head_count = head_cols // HD
    block_rows = min(512, length)
    block_count = length // block_rows
    score_scale = 1.0 / math.sqrt(HD)
    key_heads = key_flat.reshape(length, head_count, HD)
    value_heads = value_flat.reshape(length, head_count, HD)

    def one_block(totals, pieces):
        grad_keys, grad_values = totals
        query_block, seg_block, grad_block, total_block = pieces
        scores = score_block(query_block, key_heads, seg_block, segment)
        prob_full = jnp.exp(scores - total_block)
        probs_low = prob_full.astype(jnp.bfloat16)
        grad_values = grad_values + jnp.einsum(
            "hbk,bhd->khd", probs_low, grad_block, preferred_element_type=jnp.float32
        )
        grad_probs = jnp.einsum(
            "bhd,khd->hbk", grad_block, value_heads, preferred_element_type=jnp.float32
        )
        row_delta = jnp.sum(prob_full * grad_probs, axis=2, keepdims=True)
        grad_scores = (prob_full * (grad_probs - row_delta)).astype(jnp.bfloat16)
        grad_query = (
            jnp.einsum("hbk,khd->bhd", grad_scores, key_heads, preferred_element_type=jnp.float32)
            * score_scale
        )
        grad_keys = grad_keys + jnp.einsum(
            "hbk,bhd->khd", grad_scores, query_block, preferred_element_type=jnp.float32
        )
        return (
            (grad_keys, grad_values),
            grad_query.astype(jnp.bfloat16).reshape(block_rows, head_cols),
        )

    empty_sum = jnp.zeros((length, head_count, HD), jnp.float32)
    (grad_keys, grad_values), grad_query = lax.scan(
        one_block,
        (empty_sum, empty_sum),
        (
            query_heads.reshape(block_count, block_rows, head_count, HD),
            segment.reshape(block_count, block_rows),
            grad_context.reshape(block_count, block_rows, head_count, HD),
            log_total,
        ),
    )
    grad_keys = (grad_keys * score_scale).astype(jnp.bfloat16).reshape(length, head_cols)
    grad_values = grad_values.astype(jnp.bfloat16).reshape(length, head_cols)
    return (grad_query.reshape(length, head_cols), grad_keys, grad_values)


def seq_gathered_grad(left, right):
    left_all = lax.all_gather(left, "seq", axis=0, tiled=True)
    right_cols = lax.all_to_all(right, "seq", split_axis=1, concat_axis=0, tiled=True)
    partial = contract_rows(left_all, right_cols)
    return lax.psum_scatter(partial, "batch", scatter_dimension=0, tiled=True)


def batch_gathered_grad(left, right):
    left_rows = lax.all_to_all(left, "batch", split_axis=1, concat_axis=0, tiled=True)
    right_all = lax.all_gather(right, "batch", axis=0, tiled=True)
    partial = contract_rows(left_rows, right_all)
    return lax.psum_scatter(partial, "seq", scatter_dimension=1, tiled=True)


GRAD_PLAN = {"skip": "batch", "qkv": "seq", "out": "batch", "hidden": "seq", "down": "batch"}


def weight_grad(name, left, right):
    if GRAD_PLAN[name] == "seq":
        return seq_gathered_grad(left, right)
    return batch_gathered_grad(left, right)


def on_device(
    tokens,
    long_skip,
    lengths,
    skip_weight,
    skip_bias,
    attention_gain,
    attention_shift,
    qkv_weight,
    out_weight,
    out_bias,
    mlp_gain,
    mlp_shift,
    hidden_weight,
    hidden_bias,
    down_weight,
    down_bias,
    cotangent,
):
    local_rows = tokens.shape[1]
    feature_count = tokens.shape[2]
    group_len = local_rows * lax.axis_size("seq")
    joined = jnp.concatenate([tokens[0], long_skip[0]], axis=1)
    mixed = product(joined, skip_weight) + skip_bias.astype(jnp.float32)
    normed_full, first_pull = jax.vjp(
        layer_norm, mixed, attention_gain.astype(jnp.float32), attention_shift.astype(jnp.float32)
    )
    normed_one = normed_full.astype(jnp.bfloat16)
    packed = product(normed_one, qkv_weight).astype(jnp.bfloat16)
    query_tok = packed[:, :feature_count]
    key_tok = packed[:, feature_count : 2 * feature_count]
    value_tok = packed[:, 2 * feature_count :]
    query_heads, key_heads, value_heads = (
        lax.all_to_all(query_tok, "seq", split_axis=1, concat_axis=0, tiled=True),
        lax.all_to_all(key_tok, "seq", split_axis=1, concat_axis=0, tiled=True),
        lax.all_to_all(value_tok, "seq", split_axis=1, concat_axis=0, tiled=True),
    )
    segment = segments(lengths[0], group_len)
    context_heads, log_total = attend_forward(query_heads, key_heads, value_heads, segment)
    context_tok = lax.all_to_all(context_heads, "seq", split_axis=0, concat_axis=1, tiled=True)
    middle = mixed + product(context_tok, out_weight) + out_bias.astype(jnp.float32)
    second_full, second_pull = jax.vjp(
        layer_norm, middle, mlp_gain.astype(jnp.float32), mlp_shift.astype(jnp.float32)
    )
    normed_two = second_full.astype(jnp.bfloat16)
    hidden_pre = product(normed_two, hidden_weight) + hidden_bias.astype(jnp.float32)
    act_full, gelu_pull = jax.vjp(exact_gelu, hidden_pre)
    hidden_act = act_full.astype(jnp.bfloat16)
    output = (middle + product(hidden_act, down_weight) + down_bias.astype(jnp.float32)).astype(
        jnp.bfloat16
    )
    grad_out_rows = cotangent[0]
    grad_down_weight = weight_grad("down", hidden_act, grad_out_rows)
    grad_down_bias = column_sums(grad_out_rows)
    grad_act = times_transposed(grad_out_rows, down_weight)
    grad_pre = gelu_pull(grad_act)[0].astype(jnp.bfloat16)
    grad_hidden_weight = weight_grad("hidden", normed_two, grad_pre)
    grad_hidden_bias = column_sums(grad_pre)
    grad_normed_two = times_transposed(grad_pre, hidden_weight)
    grad_middle_norm, grad_mlp_gain, grad_mlp_shift = second_pull(grad_normed_two)
    grad_middle = grad_out_rows.astype(jnp.float32) + grad_middle_norm
    grad_attended = grad_middle.astype(jnp.bfloat16)
    grad_out_bias = column_sums(grad_attended)
    grad_out_weight = weight_grad("out", context_tok, grad_attended)
    grad_context = times_transposed(grad_attended, out_weight).astype(jnp.bfloat16)
    grad_context_heads = lax.all_to_all(
        grad_context, "seq", split_axis=1, concat_axis=0, tiled=True
    )
    grad_query, grad_key, grad_value = attend_backward(
        query_heads, key_heads, value_heads, segment, grad_context_heads, log_total
    )
    grad_query_tok, grad_key_tok, grad_value_tok = (
        lax.all_to_all(grad_query, "seq", split_axis=0, concat_axis=1, tiled=True),
        lax.all_to_all(grad_key, "seq", split_axis=0, concat_axis=1, tiled=True),
        lax.all_to_all(grad_value, "seq", split_axis=0, concat_axis=1, tiled=True),
    )
    grad_packed = jnp.concatenate([grad_query_tok, grad_key_tok, grad_value_tok], axis=1)
    grad_qkv_weight = weight_grad("qkv", normed_one, grad_packed)
    grad_normed_one = times_transposed(grad_packed, qkv_weight)
    grad_mixed_norm, grad_attention_gain, grad_attention_shift = first_pull(grad_normed_one)
    grad_mixed = (grad_middle + grad_mixed_norm).astype(jnp.bfloat16)
    grad_skip_bias = column_sums(grad_mixed)
    grad_skip_weight = weight_grad("skip", joined, grad_mixed)
    grad_joined = times_transposed(grad_mixed, skip_weight)
    grad_tokens = grad_joined[:, :feature_count][None]
    grad_long_skip = grad_joined[:, feature_count:][None]
    summed_weights = (grad_skip_weight, grad_qkv_weight, grad_out_weight, grad_hidden_weight, grad_down_weight)
    summed_small = lax.psum(
        (
            grad_skip_bias,
            grad_attention_gain,
            grad_attention_shift,
            grad_out_bias,
            grad_mlp_gain,
            grad_mlp_shift,
            grad_hidden_bias,
            grad_down_bias,
        ),
        ("seq", "batch"),
    )
    return (
        output[None],
        grad_tokens,
        grad_long_skip,
        summed_weights[0],
        summed_small[0],
        summed_small[1],
        summed_small[2],
        summed_weights[1],
        summed_weights[2],
        summed_small[3],
        summed_small[4],
        summed_small[5],
        summed_weights[3],
        summed_small[6],
        summed_weights[4],
        summed_small[7],
    )


def solution(mesh):
    in_specs = (
        P("batch", "seq", None),
        P("batch", "seq", None),
        P("batch", None),
        P(),
        P(),
        P(),
        P(),
        P(),
        P(),
        P(),
        P(),
        P(),
        P(),
        P(),
        P(),
        P(),
        P("batch", "seq", None),
    )
    out_specs = (
        P("batch", "seq", None),
        P("batch", "seq", None),
        P("batch", "seq", None),
        P("batch", "seq"),
        P(),
        P(),
        P(),
        P("batch", "seq"),
        P("batch", "seq"),
        P(),
        P(),
        P(),
        P("batch", "seq"),
        P(),
        P("batch", "seq"),
        P(),
    )
    return jax.shard_map(
        on_device, mesh=mesh, in_specs=in_specs, out_specs=out_specs, check_vma=False
    )
```

```python
import math

import jax
import jax.numpy as jnp
from jax import lax
from jax.sharding import PartitionSpec as P

HD = 72


norm_eps = 1e-05


def product(left, right):
    return jnp.dot(left, right, preferred_element_type=jnp.float32)


def contract_rows(left, right):
    return lax.dot_general(
        left, right, (((0,), (0,)), ((), ())), preferred_element_type=jnp.float32
    )


def times_transposed(left, right):
    return lax.dot_general(
        left, right, (((1,), (1,)), ((), ())), preferred_element_type=jnp.float32
    )


def column_sums(values):
    return jnp.sum(values.astype(jnp.float32), axis=0)


def layer_norm(inputs, gain, shift):
    mean_row = jnp.mean(inputs, axis=-1, keepdims=True)
    centred = inputs - mean_row
    spread = jnp.mean(centred * centred, axis=-1, keepdims=True)
    return centred * lax.rsqrt(spread + norm_eps) * gain + shift


def exact_gelu(inputs):
    return jax.nn.gelu(inputs, approximate=False)


def segments(row_lengths, group_len):
    ends = jnp.cumsum(row_lengths)
    places = jnp.arange(group_len, dtype=jnp.int32)
    return jnp.sum((places[:, None] >= ends[None, :]).astype(jnp.int32), axis=1)


def score_block(query_block, key_heads, seg_block, segment):
    raw = jnp.einsum("bhd,khd->hbk", query_block, key_heads, preferred_element_type=jnp.float32)
    scores = raw * (1.0 / math.sqrt(HD))
    allowed = (seg_block[:, None] == segment[None, :])[None]
    return jnp.where(allowed, scores, -jnp.inf)


def attend_forward(query_heads, key_flat, value_flat, segment):
    length, head_cols = query_heads.shape
    head_count = head_cols // HD
    block_rows = min(512, length)
    block_count = length // block_rows
    key_heads = key_flat.reshape(length, head_count, HD)
    value_heads = value_flat.reshape(length, head_count, HD)

    def one_block(pieces):
        query_block, seg_block = pieces
        scores = score_block(query_block, key_heads, seg_block, segment)
        row_max = jnp.max(scores, axis=2, keepdims=True)
        log_total = row_max + jnp.log(jnp.sum(jnp.exp(scores - row_max), axis=2, keepdims=True))
        probs_low = jnp.exp(scores - log_total).astype(jnp.bfloat16)
        context = jnp.einsum(
            "hbk,khd->bhd", probs_low, value_heads, preferred_element_type=jnp.float32
        )
        return (context.astype(jnp.bfloat16).reshape(block_rows, head_cols), log_total)

    context, log_total = lax.map(
        one_block,
        (
            query_heads.reshape(block_count, block_rows, head_count, HD),
            segment.reshape(block_count, block_rows),
        ),
    )
    return (context.reshape(length, head_cols), log_total)


def attend_backward(query_heads, key_flat, value_flat, segment, grad_context, log_total):
    length, head_cols = query_heads.shape
    head_count = head_cols // HD
    block_rows = min(512, length)
    block_count = length // block_rows
    score_scale = 1.0 / math.sqrt(HD)
    key_heads = key_flat.reshape(length, head_count, HD)
    value_heads = value_flat.reshape(length, head_count, HD)

    def one_block(totals, pieces):
        grad_keys, grad_values = totals
        query_block, seg_block, grad_block, total_block = pieces
        scores = score_block(query_block, key_heads, seg_block, segment)
        prob_full = jnp.exp(scores - total_block)
        probs_low = prob_full.astype(jnp.bfloat16)
        grad_values = grad_values + jnp.einsum(
            "hbk,bhd->khd", probs_low, grad_block, preferred_element_type=jnp.float32
        )
        grad_probs = jnp.einsum(
            "bhd,khd->hbk", grad_block, value_heads, preferred_element_type=jnp.float32
        )
        row_delta = jnp.sum(prob_full * grad_probs, axis=2, keepdims=True)
        grad_scores = (prob_full * (grad_probs - row_delta)).astype(jnp.bfloat16)
        grad_query = (
            jnp.einsum("hbk,khd->bhd", grad_scores, key_heads, preferred_element_type=jnp.float32)
            * score_scale
        )
        grad_keys = grad_keys + jnp.einsum(
            "hbk,bhd->khd", grad_scores, query_block, preferred_element_type=jnp.float32
        )
        return (
            (grad_keys, grad_values),
            grad_query.astype(jnp.bfloat16).reshape(block_rows, head_cols),
        )

    empty_sum = jnp.zeros((length, head_count, HD), jnp.float32)
    (grad_keys, grad_values), grad_query = lax.scan(
        one_block,
        (empty_sum, empty_sum),
        (
            query_heads.reshape(block_count, block_rows, head_count, HD),
            segment.reshape(block_count, block_rows),
            grad_context.reshape(block_count, block_rows, head_count, HD),
            log_total,
        ),
    )
    grad_keys = (grad_keys * score_scale).astype(jnp.bfloat16).reshape(length, head_cols)
    grad_values = grad_values.astype(jnp.bfloat16).reshape(length, head_cols)
    return (grad_query.reshape(length, head_cols), grad_keys, grad_values)


def exchange(blocks, axis):
    count = blocks.shape[0]
    me = lax.axis_index(axis)
    got = [lax.dynamic_index_in_dim(blocks, me, axis=0, keepdims=False)]
    for step in range(1, count):
        piece = lax.dynamic_index_in_dim(blocks, (me + step) % count, axis=0, keepdims=False)
        pairs = [(source, (source + step) % count) for source in range(count)]
        got.append(lax.ppermute(piece, axis, pairs))
    order = (me - jnp.arange(count)) % count
    return jnp.take(jnp.stack(got), order, axis=0)


def split_columns(values, axis):
    count = lax.axis_size(axis)
    rows, cols = values.shape
    blocks = values.reshape(rows, count, cols // count).transpose(1, 0, 2)
    return exchange(blocks, axis).reshape(count * rows, cols // count)


def seq_gathered_grad(left, right):
    left_all = lax.all_gather(left, "seq", axis=0, tiled=True)
    right_cols = split_columns(right, "seq")
    partial = contract_rows(left_all, right_cols)
    return lax.psum_scatter(partial, "batch", scatter_dimension=0, tiled=True)


def batch_gathered_grad(left, right):
    left_rows = split_columns(left, "batch")
    right_all = lax.all_gather(right, "batch", axis=0, tiled=True)
    partial = contract_rows(left_rows, right_all)
    return lax.psum_scatter(partial, "seq", scatter_dimension=1, tiled=True)


GRAD_PLAN = {"skip": "batch", "qkv": "seq", "out": "batch", "hidden": "seq", "down": "batch"}


def weight_grad(name, left, right):
    if GRAD_PLAN[name] == "seq":
        return seq_gathered_grad(left, right)
    return batch_gathered_grad(left, right)


def on_device(
    tokens,
    long_skip,
    lengths,
    skip_weight,
    skip_bias,
    attention_gain,
    attention_shift,
    qkv_weight,
    out_weight,
    out_bias,
    mlp_gain,
    mlp_shift,
    hidden_weight,
    hidden_bias,
    down_weight,
    down_bias,
    cotangent,
):
    local_rows = tokens.shape[1]
    feature_count = tokens.shape[2]
    group_len = local_rows * lax.axis_size("seq")
    joined = jnp.concatenate([tokens[0], long_skip[0]], axis=1)
    mixed = product(joined, skip_weight) + skip_bias.astype(jnp.float32)
    normed_full, first_pull = jax.vjp(
        layer_norm, mixed, attention_gain.astype(jnp.float32), attention_shift.astype(jnp.float32)
    )
    normed_one = normed_full.astype(jnp.bfloat16)
    packed = product(normed_one, qkv_weight).astype(jnp.bfloat16)
    seq_count = lax.axis_size("seq")
    packed_heads = lax.all_to_all(
        packed.reshape(local_rows, 3, seq_count, feature_count // seq_count),
        "seq",
        split_axis=2,
        concat_axis=0,
        tiled=True,
    ).reshape(group_len, 3, feature_count // seq_count)
    query_heads = packed_heads[:, 0]
    key_heads = packed_heads[:, 1]
    value_heads = packed_heads[:, 2]
    segment = segments(lengths[0], group_len)
    context_heads, log_total = attend_forward(query_heads, key_heads, value_heads, segment)
    context_tok = lax.all_to_all(context_heads, "seq", split_axis=0, concat_axis=1, tiled=True)
    middle = mixed + product(context_tok, out_weight) + out_bias.astype(jnp.float32)
    second_full, second_pull = jax.vjp(
        layer_norm, middle, mlp_gain.astype(jnp.float32), mlp_shift.astype(jnp.float32)
    )
    normed_two = second_full.astype(jnp.bfloat16)
    hidden_pre = product(normed_two, hidden_weight) + hidden_bias.astype(jnp.float32)
    act_full, gelu_pull = jax.vjp(exact_gelu, hidden_pre)
    hidden_act = act_full.astype(jnp.bfloat16)
    output = (middle + product(hidden_act, down_weight) + down_bias.astype(jnp.float32)).astype(
        jnp.bfloat16
    )
    grad_out_rows = cotangent[0]
    grad_down_weight = weight_grad("down", hidden_act, grad_out_rows)
    grad_down_bias = column_sums(grad_out_rows)
    grad_act = times_transposed(grad_out_rows, down_weight)
    grad_pre = gelu_pull(grad_act)[0].astype(jnp.bfloat16)
    grad_hidden_weight = weight_grad("hidden", normed_two, grad_pre)
    grad_hidden_bias = column_sums(grad_pre)
    grad_normed_two = times_transposed(grad_pre, hidden_weight)
    grad_middle_norm, grad_mlp_gain, grad_mlp_shift = second_pull(grad_normed_two)
    grad_middle = grad_out_rows.astype(jnp.float32) + grad_middle_norm
    grad_attended = grad_middle.astype(jnp.bfloat16)
    grad_out_bias = column_sums(grad_attended)
    grad_out_weight = weight_grad("out", context_tok, grad_attended)
    grad_context = times_transposed(grad_attended, out_weight).astype(jnp.bfloat16)
    grad_context_heads = lax.all_to_all(
        grad_context, "seq", split_axis=1, concat_axis=0, tiled=True
    )
    grad_query, grad_key, grad_value = attend_backward(
        query_heads, key_heads, value_heads, segment, grad_context_heads, log_total
    )
    grad_packed = lax.all_to_all(
        jnp.stack([grad_query, grad_key, grad_value], axis=1)[:, :, None],
        "seq",
        split_axis=0,
        concat_axis=2,
        tiled=True,
    ).reshape(local_rows, 3 * feature_count)
    grad_qkv_weight = weight_grad("qkv", normed_one, grad_packed)
    grad_normed_one = times_transposed(grad_packed, qkv_weight)
    grad_mixed_norm, grad_attention_gain, grad_attention_shift = first_pull(grad_normed_one)
    grad_mixed = (grad_middle + grad_mixed_norm).astype(jnp.bfloat16)
    grad_skip_bias = column_sums(grad_mixed)
    grad_skip_weight = weight_grad("skip", joined, grad_mixed)
    grad_joined = times_transposed(grad_mixed, skip_weight)
    grad_tokens = grad_joined[:, :feature_count][None]
    grad_long_skip = grad_joined[:, feature_count:][None]
    summed_weights = (grad_skip_weight, grad_qkv_weight, grad_out_weight, grad_hidden_weight, grad_down_weight)
    small_grads = (
        grad_skip_bias,
        grad_attention_gain,
        grad_attention_shift,
        grad_out_bias,
        grad_mlp_gain,
        grad_mlp_shift,
        grad_hidden_bias,
        grad_down_bias,
    )
    small_sizes = [piece.shape[0] for piece in small_grads]
    small_total = lax.psum(jnp.concatenate(small_grads), ("seq", "batch"))
    summed_small = []
    offset = 0
    for size in small_sizes:
        summed_small.append(small_total[offset : offset + size])
        offset += size
    return (
        output[None],
        grad_tokens,
        grad_long_skip,
        summed_weights[0],
        summed_small[0],
        summed_small[1],
        summed_small[2],
        summed_weights[1],
        summed_weights[2],
        summed_small[3],
        summed_small[4],
        summed_small[5],
        summed_weights[3],
        summed_small[6],
        summed_weights[4],
        summed_small[7],
    )


def solution(mesh):
    in_specs = (
        P("batch", "seq", None),
        P("batch", "seq", None),
        P("batch", None),
        P(),
        P(),
        P(),
        P(),
        P(),
        P(),
        P(),
        P(),
        P(),
        P(),
        P(),
        P(),
        P(),
        P("batch", "seq", None),
    )
    out_specs = (
        P("batch", "seq", None),
        P("batch", "seq", None),
        P("batch", "seq", None),
        P("batch", "seq"),
        P(),
        P(),
        P(),
        P("batch", "seq"),
        P("batch", "seq"),
        P(),
        P(),
        P(),
        P("batch", "seq"),
        P(),
        P("batch", "seq"),
        P(),
    )
    return jax.shard_map(
        on_device, mesh=mesh, in_specs=in_specs, out_specs=out_specs, check_vma=False
    )
```

```python
import math

import jax
import jax.numpy as jnp
from jax import lax
from jax.sharding import PartitionSpec as P

HD = 72


norm_eps = 1e-05


def product(left, right):
    return jnp.dot(left, right, preferred_element_type=jnp.float32)


def contract_rows(left, right):
    return lax.dot_general(
        left, right, (((0,), (0,)), ((), ())), preferred_element_type=jnp.float32
    )


def times_transposed(left, right):
    return lax.dot_general(
        left, right, (((1,), (1,)), ((), ())), preferred_element_type=jnp.float32
    )


def column_sums(values):
    return jnp.sum(values.astype(jnp.float32), axis=0)


def layer_norm(inputs, gain, shift):
    mean_row = jnp.mean(inputs, axis=-1, keepdims=True)
    centred = inputs - mean_row
    spread = jnp.mean(centred * centred, axis=-1, keepdims=True)
    return centred * lax.rsqrt(spread + norm_eps) * gain + shift


def exact_gelu(inputs):
    return jax.nn.gelu(inputs, approximate=False)


def segments(row_lengths, group_len):
    ends = jnp.cumsum(row_lengths)
    places = jnp.arange(group_len, dtype=jnp.int32)
    return jnp.sum((places[:, None] >= ends[None, :]).astype(jnp.int32), axis=1)


def score_block(query_block, key_heads, seg_block, segment):
    raw = jnp.einsum("bhd,khd->hbk", query_block, key_heads, preferred_element_type=jnp.float32)
    scores = raw * (1.0 / math.sqrt(HD))
    allowed = (seg_block[:, None] == segment[None, :])[None]
    return jnp.where(allowed, scores, -jnp.inf)


def attend_forward(query_heads, key_flat, value_flat, segment):
    length, head_cols = query_heads.shape
    head_count = head_cols // HD
    block_rows = min(512, length)
    block_count = length // block_rows
    key_heads = key_flat.reshape(length, head_count, HD)
    value_heads = value_flat.reshape(length, head_count, HD)

    def one_block(pieces):
        query_block, seg_block = pieces
        scores = score_block(query_block, key_heads, seg_block, segment)
        row_max = jnp.max(scores, axis=2, keepdims=True)
        log_total = row_max + jnp.log(jnp.sum(jnp.exp(scores - row_max), axis=2, keepdims=True))
        probs_low = jnp.exp(scores - log_total).astype(jnp.bfloat16)
        context = jnp.einsum(
            "hbk,khd->bhd", probs_low, value_heads, preferred_element_type=jnp.float32
        )
        return (context.astype(jnp.bfloat16).reshape(block_rows, head_cols), log_total)

    context, log_total = lax.map(
        one_block,
        (
            query_heads.reshape(block_count, block_rows, head_count, HD),
            segment.reshape(block_count, block_rows),
        ),
    )
    return (context.reshape(length, head_cols), log_total)


def attend_backward(query_heads, key_flat, value_flat, segment, grad_context, log_total):
    length, head_cols = query_heads.shape
    head_count = head_cols // HD
    block_rows = min(512, length)
    block_count = length // block_rows
    score_scale = 1.0 / math.sqrt(HD)
    key_heads = key_flat.reshape(length, head_count, HD)
    value_heads = value_flat.reshape(length, head_count, HD)

    def one_block(totals, pieces):
        grad_keys, grad_values = totals
        query_block, seg_block, grad_block, total_block = pieces
        scores = score_block(query_block, key_heads, seg_block, segment)
        prob_full = jnp.exp(scores - total_block)
        probs_low = prob_full.astype(jnp.bfloat16)
        grad_values = grad_values + jnp.einsum(
            "hbk,bhd->khd", probs_low, grad_block, preferred_element_type=jnp.float32
        )
        grad_probs = jnp.einsum(
            "bhd,khd->hbk", grad_block, value_heads, preferred_element_type=jnp.float32
        )
        row_delta = jnp.sum(prob_full * grad_probs, axis=2, keepdims=True)
        grad_scores = (prob_full * (grad_probs - row_delta)).astype(jnp.bfloat16)
        grad_query = (
            jnp.einsum("hbk,khd->bhd", grad_scores, key_heads, preferred_element_type=jnp.float32)
            * score_scale
        )
        grad_keys = grad_keys + jnp.einsum(
            "hbk,bhd->khd", grad_scores, query_block, preferred_element_type=jnp.float32
        )
        return (
            (grad_keys, grad_values),
            grad_query.astype(jnp.bfloat16).reshape(block_rows, head_cols),
        )

    empty_sum = jnp.zeros((length, head_count, HD), jnp.float32)
    (grad_keys, grad_values), grad_query = lax.scan(
        one_block,
        (empty_sum, empty_sum),
        (
            query_heads.reshape(block_count, block_rows, head_count, HD),
            segment.reshape(block_count, block_rows),
            grad_context.reshape(block_count, block_rows, head_count, HD),
            log_total,
        ),
    )
    grad_keys = (grad_keys * score_scale).astype(jnp.bfloat16).reshape(length, head_cols)
    grad_values = grad_values.astype(jnp.bfloat16).reshape(length, head_cols)
    return (grad_query.reshape(length, head_cols), grad_keys, grad_values)


def seq_gathered_grad(left, right):
    left_all = lax.all_gather(left, "seq", axis=0, tiled=True)
    right_cols = lax.all_to_all(right, "seq", split_axis=1, concat_axis=0, tiled=True)
    partial = contract_rows(left_all, right_cols).astype(jnp.bfloat16)
    summed = lax.psum_scatter(partial, "batch", scatter_dimension=0, tiled=True)
    return summed.astype(jnp.float32)


def batch_gathered_grad(left, right):
    left_rows = lax.all_to_all(left, "batch", split_axis=1, concat_axis=0, tiled=True)
    right_all = lax.all_gather(right, "batch", axis=0, tiled=True)
    partial = contract_rows(left_rows, right_all).astype(jnp.bfloat16)
    summed = lax.psum_scatter(partial, "seq", scatter_dimension=1, tiled=True)
    return summed.astype(jnp.float32)


GRAD_PLAN = {"skip": "batch", "qkv": "seq", "out": "batch", "hidden": "seq", "down": "batch"}


def weight_grad(name, left, right):
    if GRAD_PLAN[name] == "seq":
        return seq_gathered_grad(left, right)
    return batch_gathered_grad(left, right)


def on_device(
    tokens,
    long_skip,
    lengths,
    skip_weight,
    skip_bias,
    attention_gain,
    attention_shift,
    qkv_weight,
    out_weight,
    out_bias,
    mlp_gain,
    mlp_shift,
    hidden_weight,
    hidden_bias,
    down_weight,
    down_bias,
    cotangent,
):
    local_rows = tokens.shape[1]
    feature_count = tokens.shape[2]
    group_len = local_rows * lax.axis_size("seq")
    joined = jnp.concatenate([tokens[0], long_skip[0]], axis=1)
    mixed = product(joined, skip_weight) + skip_bias.astype(jnp.float32)
    normed_full, first_pull = jax.vjp(
        layer_norm, mixed, attention_gain.astype(jnp.float32), attention_shift.astype(jnp.float32)
    )
    normed_one = normed_full.astype(jnp.bfloat16)
    packed = product(normed_one, qkv_weight).astype(jnp.bfloat16)
    seq_count = lax.axis_size("seq")
    packed_heads = lax.all_to_all(
        packed.reshape(local_rows, 3, seq_count, feature_count // seq_count),
        "seq",
        split_axis=2,
        concat_axis=0,
        tiled=True,
    ).reshape(group_len, 3, feature_count // seq_count)
    query_heads = packed_heads[:, 0]
    key_heads = packed_heads[:, 1]
    value_heads = packed_heads[:, 2]
    segment = segments(lengths[0], group_len)
    context_heads, log_total = attend_forward(query_heads, key_heads, value_heads, segment)
    context_tok = lax.all_to_all(context_heads, "seq", split_axis=0, concat_axis=1, tiled=True)
    middle = mixed + product(context_tok, out_weight) + out_bias.astype(jnp.float32)
    second_full, second_pull = jax.vjp(
        layer_norm, middle, mlp_gain.astype(jnp.float32), mlp_shift.astype(jnp.float32)
    )
    normed_two = second_full.astype(jnp.bfloat16)
    hidden_pre = product(normed_two, hidden_weight) + hidden_bias.astype(jnp.float32)
    act_full, gelu_pull = jax.vjp(exact_gelu, hidden_pre)
    hidden_act = act_full.astype(jnp.bfloat16)
    output = (middle + product(hidden_act, down_weight) + down_bias.astype(jnp.float32)).astype(
        jnp.bfloat16
    )
    grad_out_rows = cotangent[0]
    grad_down_weight = weight_grad("down", hidden_act, grad_out_rows)
    grad_down_bias = column_sums(grad_out_rows)
    grad_act = times_transposed(grad_out_rows, down_weight)
    grad_pre = gelu_pull(grad_act)[0].astype(jnp.bfloat16)
    grad_hidden_weight = weight_grad("hidden", normed_two, grad_pre)
    grad_hidden_bias = column_sums(grad_pre)
    grad_normed_two = times_transposed(grad_pre, hidden_weight)
    grad_middle_norm, grad_mlp_gain, grad_mlp_shift = second_pull(grad_normed_two)
    grad_middle = grad_out_rows.astype(jnp.float32) + grad_middle_norm
    grad_attended = grad_middle.astype(jnp.bfloat16)
    grad_out_bias = column_sums(grad_attended)
    grad_out_weight = weight_grad("out", context_tok, grad_attended)
    grad_context = times_transposed(grad_attended, out_weight).astype(jnp.bfloat16)
    grad_context_heads = lax.all_to_all(
        grad_context, "seq", split_axis=1, concat_axis=0, tiled=True
    )
    grad_query, grad_key, grad_value = attend_backward(
        query_heads, key_heads, value_heads, segment, grad_context_heads, log_total
    )
    grad_packed = lax.all_to_all(
        jnp.stack([grad_query, grad_key, grad_value], axis=1)[:, :, None],
        "seq",
        split_axis=0,
        concat_axis=2,
        tiled=True,
    ).reshape(local_rows, 3 * feature_count)
    grad_qkv_weight = weight_grad("qkv", normed_one, grad_packed)
    grad_normed_one = times_transposed(grad_packed, qkv_weight)
    grad_mixed_norm, grad_attention_gain, grad_attention_shift = first_pull(grad_normed_one)
    grad_mixed = (grad_middle + grad_mixed_norm).astype(jnp.bfloat16)
    grad_skip_bias = column_sums(grad_mixed)
    grad_skip_weight = weight_grad("skip", joined, grad_mixed)
    grad_joined = times_transposed(grad_mixed, skip_weight)
    grad_tokens = grad_joined[:, :feature_count][None]
    grad_long_skip = grad_joined[:, feature_count:][None]
    summed_weights = (grad_skip_weight, grad_qkv_weight, grad_out_weight, grad_hidden_weight, grad_down_weight)
    small_grads = (
        grad_skip_bias,
        grad_attention_gain,
        grad_attention_shift,
        grad_out_bias,
        grad_mlp_gain,
        grad_mlp_shift,
        grad_hidden_bias,
        grad_down_bias,
    )
    small_sizes = [piece.shape[0] for piece in small_grads]
    small_total = lax.psum(jnp.concatenate(small_grads), ("seq", "batch"))
    summed_small = []
    offset = 0
    for size in small_sizes:
        summed_small.append(small_total[offset : offset + size])
        offset += size
    return (
        output[None],
        grad_tokens,
        grad_long_skip,
        summed_weights[0],
        summed_small[0],
        summed_small[1],
        summed_small[2],
        summed_weights[1],
        summed_weights[2],
        summed_small[3],
        summed_small[4],
        summed_small[5],
        summed_weights[3],
        summed_small[6],
        summed_weights[4],
        summed_small[7],
    )


def solution(mesh):
    in_specs = (
        P("batch", "seq", None),
        P("batch", "seq", None),
        P("batch", None),
        P(),
        P(),
        P(),
        P(),
        P(),
        P(),
        P(),
        P(),
        P(),
        P(),
        P(),
        P(),
        P(),
        P("batch", "seq", None),
    )
    out_specs = (
        P("batch", "seq", None),
        P("batch", "seq", None),
        P("batch", "seq", None),
        P("batch", "seq"),
        P(),
        P(),
        P(),
        P("batch", "seq"),
        P("batch", "seq"),
        P(),
        P(),
        P(),
        P("batch", "seq"),
        P(),
        P("batch", "seq"),
        P(),
    )
    return jax.shard_map(
        on_device, mesh=mesh, in_specs=in_specs, out_specs=out_specs, check_vma=False
    )
```

```python
import math

import jax
import jax.numpy as jnp
from jax import lax
from jax.sharding import PartitionSpec as P

HD = 72


norm_eps = 1e-05


def product(left, right):
    return jnp.dot(left, right, preferred_element_type=jnp.float32)


def contract_rows(left, right):
    return lax.dot_general(
        left, right, (((0,), (0,)), ((), ())), preferred_element_type=jnp.float32
    )


def times_transposed(left, right):
    return lax.dot_general(
        left, right, (((1,), (1,)), ((), ())), preferred_element_type=jnp.float32
    )


def column_sums(values):
    return jnp.sum(values.astype(jnp.float32), axis=0)


def layer_norm(inputs, gain, shift):
    mean_row = jnp.mean(inputs, axis=-1, keepdims=True)
    centred = inputs - mean_row
    spread = jnp.mean(centred * centred, axis=-1, keepdims=True)
    return centred * lax.rsqrt(spread + norm_eps) * gain + shift


def exact_gelu(inputs):
    return jax.nn.gelu(inputs, approximate=False)


def segments(row_lengths, group_len):
    ends = jnp.cumsum(row_lengths)
    places = jnp.arange(group_len, dtype=jnp.int32)
    return jnp.sum((places[:, None] >= ends[None, :]).astype(jnp.int32), axis=1)


def score_block(query_block, key_heads, seg_block, segment):
    raw = jnp.einsum("bhd,khd->hbk", query_block, key_heads, preferred_element_type=jnp.float32)
    scores = raw * (1.0 / math.sqrt(HD))
    allowed = (seg_block[:, None] == segment[None, :])[None]
    return jnp.where(allowed, scores, -jnp.inf)


def attend_forward(query_heads, key_flat, value_flat, segment):
    length, head_cols = query_heads.shape
    head_count = head_cols // HD
    block_rows = min(512, length)
    block_count = length // block_rows
    key_heads = key_flat.reshape(length, head_count, HD)
    value_heads = value_flat.reshape(length, head_count, HD)

    def one_block(pieces):
        query_block, seg_block = pieces
        scores = score_block(query_block, key_heads, seg_block, segment)
        row_max = jnp.max(scores, axis=2, keepdims=True)
        log_total = row_max + jnp.log(jnp.sum(jnp.exp(scores - row_max), axis=2, keepdims=True))
        probs_low = jnp.exp(scores - log_total).astype(jnp.bfloat16)
        context = jnp.einsum(
            "hbk,khd->bhd", probs_low, value_heads, preferred_element_type=jnp.float32
        )
        return (context.astype(jnp.bfloat16).reshape(block_rows, head_cols), log_total)

    context, log_total = lax.map(
        one_block,
        (
            query_heads.reshape(block_count, block_rows, head_count, HD),
            segment.reshape(block_count, block_rows),
        ),
    )
    return (context.reshape(length, head_cols), log_total)


def attend_backward(query_heads, key_flat, value_flat, segment, grad_context, log_total):
    length, head_cols = query_heads.shape
    head_count = head_cols // HD
    block_rows = min(512, length)
    block_count = length // block_rows
    score_scale = 1.0 / math.sqrt(HD)
    key_heads = key_flat.reshape(length, head_count, HD)
    value_heads = value_flat.reshape(length, head_count, HD)

    def one_block(totals, pieces):
        grad_keys, grad_values = totals
        query_block, seg_block, grad_block, total_block = pieces
        scores = score_block(query_block, key_heads, seg_block, segment)
        prob_full = jnp.exp(scores - total_block)
        probs_low = prob_full.astype(jnp.bfloat16)
        grad_values = grad_values + jnp.einsum(
            "hbk,bhd->khd", probs_low, grad_block, preferred_element_type=jnp.float32
        )
        grad_probs = jnp.einsum(
            "bhd,khd->hbk", grad_block, value_heads, preferred_element_type=jnp.float32
        )
        row_delta = jnp.sum(prob_full * grad_probs, axis=2, keepdims=True)
        grad_scores = (prob_full * (grad_probs - row_delta)).astype(jnp.bfloat16)
        grad_query = (
            jnp.einsum("hbk,khd->bhd", grad_scores, key_heads, preferred_element_type=jnp.float32)
            * score_scale
        )
        grad_keys = grad_keys + jnp.einsum(
            "hbk,bhd->khd", grad_scores, query_block, preferred_element_type=jnp.float32
        )
        return (
            (grad_keys, grad_values),
            grad_query.astype(jnp.bfloat16).reshape(block_rows, head_cols),
        )

    empty_sum = jnp.zeros((length, head_count, HD), jnp.float32)
    (grad_keys, grad_values), grad_query = lax.scan(
        one_block,
        (empty_sum, empty_sum),
        (
            query_heads.reshape(block_count, block_rows, head_count, HD),
            segment.reshape(block_count, block_rows),
            grad_context.reshape(block_count, block_rows, head_count, HD),
            log_total,
        ),
    )
    grad_keys = (grad_keys * score_scale).astype(jnp.bfloat16).reshape(length, head_cols)
    grad_values = grad_values.astype(jnp.bfloat16).reshape(length, head_cols)
    return (grad_query.reshape(length, head_cols), grad_keys, grad_values)


def seq_gathered_grad(left, right):
    left_all = lax.all_gather(left, "seq", axis=0, tiled=True)
    right_cols = lax.all_to_all(right, "seq", split_axis=1, concat_axis=0, tiled=True)
    partial = contract_rows(left_all, right_cols).astype(jnp.bfloat16)
    summed = lax.psum_scatter(partial, "batch", scatter_dimension=0, tiled=True)
    return summed.astype(jnp.float32)


def batch_gathered_grad(left, right):
    left_rows = lax.all_to_all(left, "batch", split_axis=1, concat_axis=0, tiled=True)
    right_all = lax.all_gather(right, "batch", axis=0, tiled=True)
    partial = contract_rows(left_rows, right_all).astype(jnp.bfloat16)
    summed = lax.psum_scatter(partial, "seq", scatter_dimension=1, tiled=True)
    return summed.astype(jnp.float32)


def qkv_grad_from_heads(left, grad_heads):
    seq_count = lax.axis_size("seq")
    me = lax.axis_index("seq")
    piece = grad_heads.shape[1] // 3
    left_all = lax.all_gather(left, "seq", axis=0, tiled=True)
    partial = contract_rows(left_all, grad_heads).astype(jnp.bfloat16)
    summed = lax.psum_scatter(partial, "batch", scatter_dimension=0, tiled=True)
    summed = summed.astype(jnp.float32)
    inverse = pow(3, -1, seq_count)
    slots = []
    for slot in range(3):
        target = ((me - slot) * inverse) % seq_count
        chunk = (3 * target + slot) // seq_count
        sent = lax.dynamic_slice_in_dim(summed, chunk * piece, piece, axis=1)
        pairs = []
        for source in range(seq_count):
            pairs.append((source, ((source - slot) * inverse) % seq_count))
        slots.append(lax.ppermute(sent, "seq", pairs))
    return jnp.concatenate(slots, axis=1)


GRAD_PLAN = {"skip": "batch", "qkv": "seq", "out": "batch", "hidden": "seq", "down": "batch"}


def weight_grad(name, left, right):
    if GRAD_PLAN[name] == "seq":
        return seq_gathered_grad(left, right)
    return batch_gathered_grad(left, right)


def on_device(
    tokens,
    long_skip,
    lengths,
    skip_weight,
    skip_bias,
    attention_gain,
    attention_shift,
    qkv_weight,
    out_weight,
    out_bias,
    mlp_gain,
    mlp_shift,
    hidden_weight,
    hidden_bias,
    down_weight,
    down_bias,
    cotangent,
):
    local_rows = tokens.shape[1]
    feature_count = tokens.shape[2]
    group_len = local_rows * lax.axis_size("seq")
    joined = jnp.concatenate([tokens[0], long_skip[0]], axis=1)
    mixed = product(joined, skip_weight) + skip_bias.astype(jnp.float32)
    normed_full, first_pull = jax.vjp(
        layer_norm, mixed, attention_gain.astype(jnp.float32), attention_shift.astype(jnp.float32)
    )
    normed_one = normed_full.astype(jnp.bfloat16)
    packed = product(normed_one, qkv_weight).astype(jnp.bfloat16)
    seq_count = lax.axis_size("seq")
    packed_heads = lax.all_to_all(
        packed.reshape(local_rows, 3, seq_count, feature_count // seq_count),
        "seq",
        split_axis=2,
        concat_axis=0,
        tiled=True,
    ).reshape(group_len, 3, feature_count // seq_count)
    query_heads = packed_heads[:, 0]
    key_heads = packed_heads[:, 1]
    value_heads = packed_heads[:, 2]
    segment = segments(lengths[0], group_len)
    context_heads, log_total = attend_forward(query_heads, key_heads, value_heads, segment)
    context_tok = lax.all_to_all(context_heads, "seq", split_axis=0, concat_axis=1, tiled=True)
    middle = mixed + product(context_tok, out_weight) + out_bias.astype(jnp.float32)
    second_full, second_pull = jax.vjp(
        layer_norm, middle, mlp_gain.astype(jnp.float32), mlp_shift.astype(jnp.float32)
    )
    normed_two = second_full.astype(jnp.bfloat16)
    hidden_pre = product(normed_two, hidden_weight) + hidden_bias.astype(jnp.float32)
    act_full, gelu_pull = jax.vjp(exact_gelu, hidden_pre)
    hidden_act = act_full.astype(jnp.bfloat16)
    output = (middle + product(hidden_act, down_weight) + down_bias.astype(jnp.float32)).astype(
        jnp.bfloat16
    )
    grad_out_rows = cotangent[0]
    grad_down_weight = weight_grad("down", hidden_act, grad_out_rows)
    grad_down_bias = column_sums(grad_out_rows)
    grad_act = times_transposed(grad_out_rows, down_weight)
    grad_pre = gelu_pull(grad_act)[0].astype(jnp.bfloat16)
    grad_hidden_weight = weight_grad("hidden", normed_two, grad_pre)
    grad_hidden_bias = column_sums(grad_pre)
    grad_normed_two = times_transposed(grad_pre, hidden_weight)
    grad_middle_norm, grad_mlp_gain, grad_mlp_shift = second_pull(grad_normed_two)
    grad_middle = grad_out_rows.astype(jnp.float32) + grad_middle_norm
    grad_attended = grad_middle.astype(jnp.bfloat16)
    grad_out_bias = column_sums(grad_attended)
    grad_out_weight = weight_grad("out", context_tok, grad_attended)
    grad_context = times_transposed(grad_attended, out_weight).astype(jnp.bfloat16)
    grad_context_heads = lax.all_to_all(
        grad_context, "seq", split_axis=1, concat_axis=0, tiled=True
    )
    grad_query, grad_key, grad_value = attend_backward(
        query_heads, key_heads, value_heads, segment, grad_context_heads, log_total
    )
    grad_packed = jnp.concatenate(
        [
            lax.all_to_all(grad_query, "seq", split_axis=0, concat_axis=1, tiled=True),
            lax.all_to_all(grad_key, "seq", split_axis=0, concat_axis=1, tiled=True),
            lax.all_to_all(grad_value, "seq", split_axis=0, concat_axis=1, tiled=True),
        ],
        axis=1,
    )
    grad_qkv_weight = qkv_grad_from_heads(
        normed_one, jnp.concatenate([grad_query, grad_key, grad_value], axis=1)
    )
    grad_normed_one = times_transposed(grad_packed, qkv_weight)
    grad_mixed_norm, grad_attention_gain, grad_attention_shift = first_pull(grad_normed_one)
    grad_mixed = (grad_middle + grad_mixed_norm).astype(jnp.bfloat16)
    grad_skip_bias = column_sums(grad_mixed)
    grad_skip_weight = weight_grad("skip", joined, grad_mixed)
    grad_joined = times_transposed(grad_mixed, skip_weight)
    grad_tokens = grad_joined[:, :feature_count][None]
    grad_long_skip = grad_joined[:, feature_count:][None]
    summed_weights = (grad_skip_weight, grad_qkv_weight, grad_out_weight, grad_hidden_weight, grad_down_weight)
    small_grads = (
        grad_skip_bias,
        grad_attention_gain,
        grad_attention_shift,
        grad_out_bias,
        grad_mlp_gain,
        grad_mlp_shift,
        grad_hidden_bias,
        grad_down_bias,
    )
    small_sizes = [piece.shape[0] for piece in small_grads]
    small_total = lax.psum(jnp.concatenate(small_grads), ("seq", "batch"))
    summed_small = []
    offset = 0
    for size in small_sizes:
        summed_small.append(small_total[offset : offset + size])
        offset += size
    return (
        output[None],
        grad_tokens,
        grad_long_skip,
        summed_weights[0],
        summed_small[0],
        summed_small[1],
        summed_small[2],
        summed_weights[1],
        summed_weights[2],
        summed_small[3],
        summed_small[4],
        summed_small[5],
        summed_weights[3],
        summed_small[6],
        summed_weights[4],
        summed_small[7],
    )


def solution(mesh):
    in_specs = (
        P("batch", "seq", None),
        P("batch", "seq", None),
        P("batch", None),
        P(),
        P(),
        P(),
        P(),
        P(),
        P(),
        P(),
        P(),
        P(),
        P(),
        P(),
        P(),
        P(),
        P("batch", "seq", None),
    )
    out_specs = (
        P("batch", "seq", None),
        P("batch", "seq", None),
        P("batch", "seq", None),
        P("batch", "seq"),
        P(),
        P(),
        P(),
        P("batch", "seq"),
        P("batch", "seq"),
        P(),
        P(),
        P(),
        P("batch", "seq"),
        P(),
        P("batch", "seq"),
        P(),
    )
    return jax.shard_map(
        on_device, mesh=mesh, in_specs=in_specs, out_specs=out_specs, check_vma=False
    )
```

```python
import math

import jax
import jax.numpy as jnp
from jax import lax
from jax.sharding import PartitionSpec as P


HD = 72


norm_eps = 1e-05


def product(left, right):
    return jnp.dot(left, right, preferred_element_type=jnp.float32)


def contract_rows(left, right):
    return lax.dot_general(
        left, right, (((0,), (0,)), ((), ())), preferred_element_type=jnp.float32
    )


def times_transposed(left, right):
    return lax.dot_general(
        left, right, (((1,), (1,)), ((), ())), preferred_element_type=jnp.float32
    )


def column_sums(values):
    return jnp.sum(values.astype(jnp.float32), axis=0)


def layer_norm(inputs, gain, shift):
    mean_row = jnp.mean(inputs, axis=-1, keepdims=True)
    centred = inputs - mean_row
    spread = jnp.mean(centred * centred, axis=-1, keepdims=True)
    return centred * lax.rsqrt(spread + norm_eps) * gain + shift


def exact_gelu(inputs):
    return jax.nn.gelu(inputs, approximate=False)


def segments(row_lengths, group_len):
    ends = jnp.cumsum(row_lengths)
    places = jnp.arange(group_len, dtype=jnp.int32)
    return jnp.sum((places[:, None] >= ends[None, :]).astype(jnp.int32), axis=1)


def score_block(query_block, key_heads, seg_block, segment):
    raw = jnp.einsum("bhd,khd->hbk", query_block, key_heads, preferred_element_type=jnp.float32)
    scores = raw * (1.0 / math.sqrt(HD))
    allowed = (seg_block[:, None] == segment[None, :])[None]
    return jnp.where(allowed, scores, -jnp.inf)


def attend_forward(query_heads, key_flat, value_flat, segment):
    length, head_cols = query_heads.shape
    head_count = head_cols // HD
    block_rows = min(512, length)
    block_count = length // block_rows
    key_heads = key_flat.reshape(length, head_count, HD)
    value_heads = value_flat.reshape(length, head_count, HD)

    def one_block(pieces):
        query_block, seg_block = pieces
        scores = score_block(query_block, key_heads, seg_block, segment)
        row_max = jnp.max(scores, axis=2, keepdims=True)
        log_total = row_max + jnp.log(jnp.sum(jnp.exp(scores - row_max), axis=2, keepdims=True))
        probs_low = jnp.exp(scores - log_total).astype(jnp.bfloat16)
        context = jnp.einsum(
            "hbk,khd->bhd", probs_low, value_heads, preferred_element_type=jnp.float32
        )
        return (context.astype(jnp.bfloat16).reshape(block_rows, head_cols), log_total)

    context, log_total = lax.map(
        one_block,
        (
            query_heads.reshape(block_count, block_rows, head_count, HD),
            segment.reshape(block_count, block_rows),
        ),
    )
    return (context.reshape(length, head_cols), log_total)


def attend_backward(query_heads, key_flat, value_flat, segment, grad_context, log_total):
    length, head_cols = query_heads.shape
    head_count = head_cols // HD
    block_rows = min(512, length)
    block_count = length // block_rows
    score_scale = 1.0 / math.sqrt(HD)
    key_heads = key_flat.reshape(length, head_count, HD)
    value_heads = value_flat.reshape(length, head_count, HD)

    def one_block(totals, pieces):
        grad_keys, grad_values = totals
        query_block, seg_block, grad_block, total_block = pieces
        scores = score_block(query_block, key_heads, seg_block, segment)
        prob_full = jnp.exp(scores - total_block)
        probs_low = prob_full.astype(jnp.bfloat16)
        grad_values = grad_values + jnp.einsum(
            "hbk,bhd->khd", probs_low, grad_block, preferred_element_type=jnp.float32
        )
        grad_probs = jnp.einsum(
            "bhd,khd->hbk", grad_block, value_heads, preferred_element_type=jnp.float32
        )
        row_delta = jnp.sum(prob_full * grad_probs, axis=2, keepdims=True)
        grad_scores = (prob_full * (grad_probs - row_delta)).astype(jnp.bfloat16)
        grad_query = (
            jnp.einsum("hbk,khd->bhd", grad_scores, key_heads, preferred_element_type=jnp.float32)
            * score_scale
        )
        grad_keys = grad_keys + jnp.einsum(
            "hbk,bhd->khd", grad_scores, query_block, preferred_element_type=jnp.float32
        )
        return (
            (grad_keys, grad_values),
            grad_query.astype(jnp.bfloat16).reshape(block_rows, head_cols),
        )

    empty_sum = jnp.zeros((length, head_count, HD), jnp.float32)
    (grad_keys, grad_values), grad_query = lax.scan(
        one_block,
        (empty_sum, empty_sum),
        (
            query_heads.reshape(block_count, block_rows, head_count, HD),
            segment.reshape(block_count, block_rows),
            grad_context.reshape(block_count, block_rows, head_count, HD),
            log_total,
        ),
    )
    grad_keys = (grad_keys * score_scale).astype(jnp.bfloat16).reshape(length, head_cols)
    grad_values = grad_values.astype(jnp.bfloat16).reshape(length, head_cols)
    return (grad_query.reshape(length, head_cols), grad_keys, grad_values)


def scatter_sum(partial, axis, dim):
    count = lax.axis_size(axis)
    shape = partial.shape
    pieces = partial.reshape(shape[:dim] + (count, shape[dim] // count) + shape[dim + 1 :])
    swapped = lax.all_to_all(pieces, axis, split_axis=dim, concat_axis=dim, tiled=True)
    return jnp.sum(swapped.astype(jnp.float32), axis=dim)


EXCHANGE_SUM = ("hidden", "skip")


def seq_gathered_grad(left, right, by_exchange):
    left_all = lax.all_gather(left, "seq", axis=0, tiled=True)
    right_cols = lax.all_to_all(right, "seq", split_axis=1, concat_axis=0, tiled=True)
    partial = contract_rows(left_all, right_cols).astype(jnp.bfloat16)
    if by_exchange:
        return scatter_sum(partial, "batch", 0)
    summed = lax.psum_scatter(partial, "batch", scatter_dimension=0, tiled=True)
    return summed.astype(jnp.float32)


def batch_gathered_grad(left, right, by_exchange):
    left_rows = lax.all_to_all(left, "batch", split_axis=1, concat_axis=0, tiled=True)
    right_all = lax.all_gather(right, "batch", axis=0, tiled=True)
    partial = contract_rows(left_rows, right_all).astype(jnp.bfloat16)
    if by_exchange:
        return scatter_sum(partial, "seq", 1)
    summed = lax.psum_scatter(partial, "seq", scatter_dimension=1, tiled=True)
    return summed.astype(jnp.float32)


def qkv_grad_from_heads(left, grad_heads):
    seq_count = lax.axis_size("seq")
    me = lax.axis_index("seq")
    piece = grad_heads.shape[1] // 3
    left_all = lax.all_gather(left, "seq", axis=0, tiled=True)
    partial = contract_rows(left_all, grad_heads).astype(jnp.bfloat16)
    summed = lax.psum_scatter(partial, "batch", scatter_dimension=0, tiled=True)
    summed = summed.astype(jnp.float32)
    inverse = pow(3, -1, seq_count)
    slots = []
    for slot in range(3):
        target = ((me - slot) * inverse) % seq_count
        chunk = (3 * target + slot) // seq_count
        sent = lax.dynamic_slice_in_dim(summed, chunk * piece, piece, axis=1)
        pairs = []
        for source in range(seq_count):
            pairs.append((source, ((source - slot) * inverse) % seq_count))
        slots.append(lax.ppermute(sent, "seq", pairs))
    return jnp.concatenate(slots, axis=1)


GRAD_PLAN = {"skip": "batch", "qkv": "seq", "out": "batch", "hidden": "seq", "down": "batch"}


def weight_grad(name, left, right):
    if GRAD_PLAN[name] == "seq":
        return seq_gathered_grad(left, right, name in EXCHANGE_SUM)
    return batch_gathered_grad(left, right, name in EXCHANGE_SUM)


def block(
    tokens,
    long_skip,
    lengths,
    skip_weight,
    skip_bias,
    attention_gain,
    attention_shift,
    qkv_weight,
    out_weight,
    out_bias,
    mlp_gain,
    mlp_shift,
    hidden_weight,
    hidden_bias,
    down_weight,
    down_bias,
    cotangent,
):
    local_rows = tokens.shape[1]
    feature_count = tokens.shape[2]
    group_len = local_rows * lax.axis_size("seq")
    joined = jnp.concatenate([tokens[0], long_skip[0]], axis=1)
    mixed = product(joined, skip_weight) + skip_bias.astype(jnp.float32)
    normed_full, first_pull = jax.vjp(
        layer_norm, mixed, attention_gain.astype(jnp.float32), attention_shift.astype(jnp.float32)
    )
    normed_one = normed_full.astype(jnp.bfloat16)
    packed = product(normed_one, qkv_weight).astype(jnp.bfloat16)
    seq_count = lax.axis_size("seq")
    packed_heads = lax.all_to_all(
        packed.reshape(local_rows, 3, seq_count, feature_count // seq_count),
        "seq",
        split_axis=2,
        concat_axis=0,
        tiled=True,
    ).reshape(group_len, 3, feature_count // seq_count)
    query_heads = packed_heads[:, 0]
    key_heads = packed_heads[:, 1]
    value_heads = packed_heads[:, 2]
    segment = segments(lengths[0], group_len)
    context_heads, log_total = attend_forward(query_heads, key_heads, value_heads, segment)
    context_tok = lax.all_to_all(context_heads, "seq", split_axis=0, concat_axis=1, tiled=True)
    middle = mixed + product(context_tok, out_weight) + out_bias.astype(jnp.float32)
    second_full, second_pull = jax.vjp(
        layer_norm, middle, mlp_gain.astype(jnp.float32), mlp_shift.astype(jnp.float32)
    )
    normed_two = second_full.astype(jnp.bfloat16)
    hidden_pre = product(normed_two, hidden_weight) + hidden_bias.astype(jnp.float32)
    act_full, gelu_pull = jax.vjp(exact_gelu, hidden_pre)
    hidden_act = act_full.astype(jnp.bfloat16)
    output = (middle + product(hidden_act, down_weight) + down_bias.astype(jnp.float32)).astype(
        jnp.bfloat16
    )
    grad_out_rows = cotangent[0]
    grad_down_weight = weight_grad("down", hidden_act, grad_out_rows)
    grad_down_bias = column_sums(grad_out_rows)
    grad_act = times_transposed(grad_out_rows, down_weight)
    grad_pre = gelu_pull(grad_act)[0].astype(jnp.bfloat16)
    grad_hidden_weight = weight_grad("hidden", normed_two, grad_pre)
    grad_hidden_bias = column_sums(grad_pre)
    grad_normed_two = times_transposed(grad_pre, hidden_weight)
    grad_middle_norm, grad_mlp_gain, grad_mlp_shift = second_pull(grad_normed_two)
    grad_middle = grad_out_rows.astype(jnp.float32) + grad_middle_norm
    grad_attended = grad_middle.astype(jnp.bfloat16)
    grad_out_bias = column_sums(grad_attended)
    grad_out_weight = weight_grad("out", context_tok, grad_attended)
    grad_context = times_transposed(grad_attended, out_weight).astype(jnp.bfloat16)
    grad_context_heads = lax.all_to_all(
        grad_context, "seq", split_axis=1, concat_axis=0, tiled=True
    )
    grad_query, grad_key, grad_value = attend_backward(
        query_heads, key_heads, value_heads, segment, grad_context_heads, log_total
    )
    grad_packed = jnp.concatenate(
        [
            lax.all_to_all(grad_query, "seq", split_axis=0, concat_axis=1, tiled=True),
            lax.all_to_all(grad_key, "seq", split_axis=0, concat_axis=1, tiled=True),
            lax.all_to_all(grad_value, "seq", split_axis=0, concat_axis=1, tiled=True),
        ],
        axis=1,
    )
    grad_qkv_weight = qkv_grad_from_heads(
        normed_one, jnp.concatenate([grad_query, grad_key, grad_value], axis=1)
    )
    grad_normed_one = times_transposed(grad_packed, qkv_weight)
    grad_mixed_norm, grad_attention_gain, grad_attention_shift = first_pull(grad_normed_one)
    grad_mixed = (grad_middle + grad_mixed_norm).astype(jnp.bfloat16)
    grad_skip_bias = column_sums(grad_mixed)
    grad_skip_weight = weight_grad("skip", joined, grad_mixed)
    grad_joined = times_transposed(grad_mixed, skip_weight)
    grad_tokens = grad_joined[:, :feature_count][None]
    grad_long_skip = grad_joined[:, feature_count:][None]
    summed_weights = (grad_skip_weight, grad_qkv_weight, grad_out_weight, grad_hidden_weight, grad_down_weight)
    small_grads = (
        grad_skip_bias,
        grad_attention_gain,
        grad_attention_shift,
        grad_out_bias,
        grad_mlp_gain,
        grad_mlp_shift,
        grad_hidden_bias,
        grad_down_bias,
    )
    small_sizes = [piece.shape[0] for piece in small_grads]
    small_total = lax.psum(jnp.concatenate(small_grads), ("seq", "batch"))
    summed_small = []
    offset = 0
    for size in small_sizes:
        summed_small.append(small_total[offset : offset + size])
        offset += size
    return (
        output[None],
        grad_tokens,
        grad_long_skip,
        summed_weights[0],
        summed_small[0],
        summed_small[1],
        summed_small[2],
        summed_weights[1],
        summed_weights[2],
        summed_small[3],
        summed_small[4],
        summed_small[5],
        summed_weights[3],
        summed_small[6],
        summed_weights[4],
        summed_small[7],
    )


def solution(mesh):
    in_specs = (
        P("batch", "seq", None),
        P("batch", "seq", None),
        P("batch", None),
        P(),
        P(),
        P(),
        P(),
        P(),
        P(),
        P(),
        P(),
        P(),
        P(),
        P(),
        P(),
        P(),
        P("batch", "seq", None),
    )
    out_specs = (
        P("batch", "seq", None),
        P("batch", "seq", None),
        P("batch", "seq", None),
        P("batch", "seq"),
        P(),
        P(),
        P(),
        P("batch", "seq"),
        P("batch", "seq"),
        P(),
        P(),
        P(),
        P("batch", "seq"),
        P(),
        P("batch", "seq"),
        P(),
    )
    return jax.shard_map(block, mesh=mesh, in_specs=in_specs, out_specs=out_specs, check_vma=False)
```

```python
import math

import jax
import jax.numpy as jnp
from jax import lax
from jax.sharding import PartitionSpec as P


HD = 72
ATTENTION_BLOCK = 256


norm_eps = 1e-05


def product(left, right):
    return jnp.dot(left, right, preferred_element_type=jnp.float32)


def contract_rows(left, right):
    return lax.dot_general(
        left, right, (((0,), (0,)), ((), ())), preferred_element_type=jnp.float32
    )


def times_transposed(left, right):
    return lax.dot_general(
        left, right, (((1,), (1,)), ((), ())), preferred_element_type=jnp.float32
    )


def column_sums(values):
    return jnp.sum(values.astype(jnp.float32), axis=0)


def layer_norm(inputs, gain, shift):
    mean_row = jnp.mean(inputs, axis=-1, keepdims=True)
    centred = inputs - mean_row
    spread = jnp.mean(centred * centred, axis=-1, keepdims=True)
    return centred * lax.rsqrt(spread + norm_eps) * gain + shift


def exact_gelu(inputs):
    return jax.nn.gelu(inputs, approximate=False)


def segments(row_lengths, group_len):
    ends = jnp.cumsum(row_lengths)
    places = jnp.arange(group_len, dtype=jnp.int32)
    return jnp.sum((places[:, None] >= ends[None, :]).astype(jnp.int32), axis=1)


def score_block(query_block, key_heads, seg_block, segment):
    raw = jnp.einsum("bhd,khd->hbk", query_block, key_heads, preferred_element_type=jnp.float32)
    scores = raw * (1.0 / math.sqrt(HD))
    allowed = (seg_block[:, None] == segment[None, :])[None]
    return jnp.where(allowed, scores, -jnp.inf)


def attend_forward(query_heads, key_flat, value_flat, segment):
    length, head_cols = query_heads.shape
    head_count = head_cols // HD
    block_rows = min(ATTENTION_BLOCK, length)
    block_count = length // block_rows
    key_heads = key_flat.reshape(length, head_count, HD)
    value_heads = value_flat.reshape(length, head_count, HD)

    def one_block(pieces):
        query_block, seg_block = pieces
        scores = score_block(query_block, key_heads, seg_block, segment)
        row_max = jnp.max(scores, axis=2, keepdims=True)
        log_total = row_max + jnp.log(jnp.sum(jnp.exp(scores - row_max), axis=2, keepdims=True))
        probs_low = jnp.exp(scores - log_total).astype(jnp.bfloat16)
        context = jnp.einsum(
            "hbk,khd->bhd", probs_low, value_heads, preferred_element_type=jnp.float32
        )
        return (context.astype(jnp.bfloat16).reshape(block_rows, head_cols), log_total)

    context, log_total = lax.map(
        one_block,
        (
            query_heads.reshape(block_count, block_rows, head_count, HD),
            segment.reshape(block_count, block_rows),
        ),
    )
    return (context.reshape(length, head_cols), log_total)


def attend_backward(query_heads, key_flat, value_flat, segment, grad_context, log_total):
    length, head_cols = query_heads.shape
    head_count = head_cols // HD
    block_rows = min(ATTENTION_BLOCK, length)
    block_count = length // block_rows
    score_scale = 1.0 / math.sqrt(HD)
    key_heads = key_flat.reshape(length, head_count, HD)
    value_heads = value_flat.reshape(length, head_count, HD)

    def one_block(totals, pieces):
        grad_keys, grad_values = totals
        query_block, seg_block, grad_block, total_block = pieces
        scores = score_block(query_block, key_heads, seg_block, segment)
        prob_full = jnp.exp(scores - total_block)
        probs_low = prob_full.astype(jnp.bfloat16)
        grad_values = grad_values + jnp.einsum(
            "hbk,bhd->khd", probs_low, grad_block, preferred_element_type=jnp.float32
        )
        grad_probs = jnp.einsum(
            "bhd,khd->hbk", grad_block, value_heads, preferred_element_type=jnp.float32
        )
        row_delta = jnp.sum(prob_full * grad_probs, axis=2, keepdims=True)
        grad_scores = (prob_full * (grad_probs - row_delta)).astype(jnp.bfloat16)
        grad_query = (
            jnp.einsum("hbk,khd->bhd", grad_scores, key_heads, preferred_element_type=jnp.float32)
            * score_scale
        )
        grad_keys = grad_keys + jnp.einsum(
            "hbk,bhd->khd", grad_scores, query_block, preferred_element_type=jnp.float32
        )
        return (
            (grad_keys, grad_values),
            grad_query.astype(jnp.bfloat16).reshape(block_rows, head_cols),
        )

    empty_sum = jnp.zeros((length, head_count, HD), jnp.float32)
    (grad_keys, grad_values), grad_query = lax.scan(
        one_block,
        (empty_sum, empty_sum),
        (
            query_heads.reshape(block_count, block_rows, head_count, HD),
            segment.reshape(block_count, block_rows),
            grad_context.reshape(block_count, block_rows, head_count, HD),
            log_total,
        ),
    )
    grad_keys = (grad_keys * score_scale).astype(jnp.bfloat16).reshape(length, head_cols)
    grad_values = grad_values.astype(jnp.bfloat16).reshape(length, head_cols)
    return (grad_query.reshape(length, head_cols), grad_keys, grad_values)


def seq_gathered_grad(left, right):
    left_all = lax.all_gather(left, "seq", axis=0, tiled=True)
    right_cols = lax.all_to_all(right, "seq", split_axis=1, concat_axis=0, tiled=True)
    partial = contract_rows(left_all, right_cols).astype(jnp.bfloat16)
    summed = lax.psum_scatter(partial, "batch", scatter_dimension=0, tiled=True)
    return summed.astype(jnp.float32)


def batch_gathered_grad(left, right):
    left_rows = lax.all_to_all(left, "batch", split_axis=1, concat_axis=0, tiled=True)
    right_all = lax.all_gather(right, "batch", axis=0, tiled=True)
    partial = contract_rows(left_rows, right_all).astype(jnp.bfloat16)
    summed = lax.psum_scatter(partial, "seq", scatter_dimension=1, tiled=True)
    return summed.astype(jnp.float32)


def qkv_grad_from_heads(left, grad_heads):
    seq_count = lax.axis_size("seq")
    me = lax.axis_index("seq")
    piece = grad_heads.shape[1] // 3
    left_all = lax.all_gather(left, "seq", axis=0, tiled=True)
    partial = contract_rows(left_all, grad_heads).astype(jnp.bfloat16)
    summed = lax.psum_scatter(partial, "batch", scatter_dimension=0, tiled=True)
    summed = summed.astype(jnp.float32)
    inverse = pow(3, -1, seq_count)
    slots = []
    for slot in range(3):
        target = ((me - slot) * inverse) % seq_count
        chunk = (3 * target + slot) // seq_count
        sent = lax.dynamic_slice_in_dim(summed, chunk * piece, piece, axis=1)
        pairs = []
        for source in range(seq_count):
            pairs.append((source, ((source - slot) * inverse) % seq_count))
        slots.append(lax.ppermute(sent, "seq", pairs))
    return jnp.concatenate(slots, axis=1)


GRAD_PLAN = {"skip": "batch", "qkv": "seq", "out": "batch", "hidden": "seq", "down": "batch"}


def weight_grad(name, left, right):
    if GRAD_PLAN[name] == "seq":
        return seq_gathered_grad(left, right)
    return batch_gathered_grad(left, right)


def block(
    tokens,
    long_skip,
    lengths,
    skip_weight,
    skip_bias,
    attention_gain,
    attention_shift,
    qkv_weight,
    out_weight,
    out_bias,
    mlp_gain,
    mlp_shift,
    hidden_weight,
    hidden_bias,
    down_weight,
    down_bias,
    cotangent,
):
    local_rows = tokens.shape[1]
    feature_count = tokens.shape[2]
    group_len = local_rows * lax.axis_size("seq")
    joined = jnp.concatenate([tokens[0], long_skip[0]], axis=1)
    mixed = product(joined, skip_weight) + skip_bias.astype(jnp.float32)
    normed_full, first_pull = jax.vjp(
        layer_norm, mixed, attention_gain.astype(jnp.float32), attention_shift.astype(jnp.float32)
    )
    normed_one = normed_full.astype(jnp.bfloat16)
    packed = product(normed_one, qkv_weight).astype(jnp.bfloat16)
    seq_count = lax.axis_size("seq")
    packed_heads = lax.all_to_all(
        packed.reshape(local_rows, 3, seq_count, feature_count // seq_count),
        "seq",
        split_axis=2,
        concat_axis=0,
        tiled=True,
    ).reshape(group_len, 3, feature_count // seq_count)
    query_heads = packed_heads[:, 0]
    key_heads = packed_heads[:, 1]
    value_heads = packed_heads[:, 2]
    segment = segments(lengths[0], group_len)
    context_heads, log_total = attend_forward(query_heads, key_heads, value_heads, segment)
    context_tok = lax.all_to_all(context_heads, "seq", split_axis=0, concat_axis=1, tiled=True)
    middle = mixed + product(context_tok, out_weight) + out_bias.astype(jnp.float32)
    second_full, second_pull = jax.vjp(
        layer_norm, middle, mlp_gain.astype(jnp.float32), mlp_shift.astype(jnp.float32)
    )
    normed_two = second_full.astype(jnp.bfloat16)
    hidden_pre = product(normed_two, hidden_weight) + hidden_bias.astype(jnp.float32)
    act_full, gelu_pull = jax.vjp(exact_gelu, hidden_pre)
    hidden_act = act_full.astype(jnp.bfloat16)
    output = (middle + product(hidden_act, down_weight) + down_bias.astype(jnp.float32)).astype(
        jnp.bfloat16
    )
    grad_out_rows = cotangent[0]
    grad_down_weight = weight_grad("down", hidden_act, grad_out_rows)
    grad_down_bias = column_sums(grad_out_rows)
    grad_act = times_transposed(grad_out_rows, down_weight)
    grad_pre = gelu_pull(grad_act)[0].astype(jnp.bfloat16)
    grad_hidden_weight = weight_grad("hidden", normed_two, grad_pre)
    grad_hidden_bias = column_sums(grad_pre)
    grad_normed_two = times_transposed(grad_pre, hidden_weight)
    grad_middle_norm, grad_mlp_gain, grad_mlp_shift = second_pull(grad_normed_two)
    grad_middle = grad_out_rows.astype(jnp.float32) + grad_middle_norm
    grad_attended = grad_middle.astype(jnp.bfloat16)
    grad_out_bias = column_sums(grad_attended)
    grad_out_weight = weight_grad("out", context_tok, grad_attended)
    grad_context = times_transposed(grad_attended, out_weight).astype(jnp.bfloat16)
    grad_context_heads = lax.all_to_all(
        grad_context, "seq", split_axis=1, concat_axis=0, tiled=True
    )
    grad_query, grad_key, grad_value = attend_backward(
        query_heads, key_heads, value_heads, segment, grad_context_heads, log_total
    )
    grad_packed = jnp.concatenate(
        [
            lax.all_to_all(grad_query, "seq", split_axis=0, concat_axis=1, tiled=True),
            lax.all_to_all(grad_key, "seq", split_axis=0, concat_axis=1, tiled=True),
            lax.all_to_all(grad_value, "seq", split_axis=0, concat_axis=1, tiled=True),
        ],
        axis=1,
    )
    grad_qkv_weight = qkv_grad_from_heads(
        normed_one, jnp.concatenate([grad_query, grad_key, grad_value], axis=1)
    )
    grad_normed_one = times_transposed(grad_packed, qkv_weight)
    grad_mixed_norm, grad_attention_gain, grad_attention_shift = first_pull(grad_normed_one)
    grad_mixed = (grad_middle + grad_mixed_norm).astype(jnp.bfloat16)
    grad_skip_bias = column_sums(grad_mixed)
    grad_skip_weight = weight_grad("skip", joined, grad_mixed)
    grad_joined = times_transposed(grad_mixed, skip_weight)
    grad_tokens = grad_joined[:, :feature_count][None]
    grad_long_skip = grad_joined[:, feature_count:][None]
    summed_weights = (grad_skip_weight, grad_qkv_weight, grad_out_weight, grad_hidden_weight, grad_down_weight)
    small_grads = (
        grad_skip_bias,
        grad_attention_gain,
        grad_attention_shift,
        grad_out_bias,
        grad_mlp_gain,
        grad_mlp_shift,
        grad_hidden_bias,
        grad_down_bias,
    )
    small_sizes = [piece.shape[0] for piece in small_grads]
    small_total = lax.psum(jnp.concatenate(small_grads), ("seq", "batch"))
    summed_small = []
    offset = 0
    for size in small_sizes:
        summed_small.append(small_total[offset : offset + size])
        offset += size
    return (
        output[None],
        grad_tokens,
        grad_long_skip,
        summed_weights[0],
        summed_small[0],
        summed_small[1],
        summed_small[2],
        summed_weights[1],
        summed_weights[2],
        summed_small[3],
        summed_small[4],
        summed_small[5],
        summed_weights[3],
        summed_small[6],
        summed_weights[4],
        summed_small[7],
    )


def solution(mesh):
    in_specs = (
        P("batch", "seq", None),
        P("batch", "seq", None),
        P("batch", None),
        P(),
        P(),
        P(),
        P(),
        P(),
        P(),
        P(),
        P(),
        P(),
        P(),
        P(),
        P(),
        P(),
        P("batch", "seq", None),
    )
    out_specs = (
        P("batch", "seq", None),
        P("batch", "seq", None),
        P("batch", "seq", None),
        P("batch", "seq"),
        P(),
        P(),
        P(),
        P("batch", "seq"),
        P("batch", "seq"),
        P(),
        P(),
        P(),
        P("batch", "seq"),
        P(),
        P("batch", "seq"),
        P(),
    )
    return jax.shard_map(block, mesh=mesh, in_specs=in_specs, out_specs=out_specs, check_vma=False)
```

```python
import math

import jax
import jax.numpy as jnp
from jax import lax
from jax.sharding import PartitionSpec as P


HD = 72


norm_eps = 1e-05


def product(left, right):
    return jnp.dot(left, right, preferred_element_type=jnp.float32)


def contract_rows(left, right):
    return lax.dot_general(
        left, right, (((0,), (0,)), ((), ())), preferred_element_type=jnp.float32
    )


def times_transposed(left, right):
    return lax.dot_general(
        left, right, (((1,), (1,)), ((), ())), preferred_element_type=jnp.float32
    )


def column_sums(values):
    return jnp.sum(values.astype(jnp.float32), axis=0)


def layer_norm(inputs, gain, shift):
    mean_row = jnp.mean(inputs, axis=-1, keepdims=True)
    centred = inputs - mean_row
    spread = jnp.mean(centred * centred, axis=-1, keepdims=True)
    return centred * lax.rsqrt(spread + norm_eps) * gain + shift


def exact_gelu(inputs):
    return jax.nn.gelu(inputs, approximate=False)


def segments(row_lengths, group_len):
    ends = jnp.cumsum(row_lengths)
    places = jnp.arange(group_len, dtype=jnp.int32)
    return jnp.sum((places[:, None] >= ends[None, :]).astype(jnp.int32), axis=1)


def score_block(query_block, key_heads, seg_block, segment):
    raw = jnp.einsum("bhd,khd->hbk", query_block, key_heads, preferred_element_type=jnp.float32)
    scores = raw * (1.0 / math.sqrt(HD))
    allowed = (seg_block[:, None] == segment[None, :])[None]
    return jnp.where(allowed, scores, -jnp.inf)


def attend_forward(query_heads, key_flat, value_flat, segment):
    length, head_cols = query_heads.shape
    head_count = head_cols // HD
    block_rows = min(512, length)
    block_count = length // block_rows
    key_heads = key_flat.reshape(length, head_count, HD)
    value_heads = value_flat.reshape(length, head_count, HD)

    def one_block(pieces):
        query_block, seg_block = pieces
        scores = score_block(query_block, key_heads, seg_block, segment)
        row_max = jnp.max(scores, axis=2, keepdims=True)
        log_total = row_max + jnp.log(jnp.sum(jnp.exp(scores - row_max), axis=2, keepdims=True))
        probs_low = jnp.exp(scores - log_total).astype(jnp.bfloat16)
        context = jnp.einsum(
            "hbk,khd->bhd", probs_low, value_heads, preferred_element_type=jnp.float32
        )
        return (context.astype(jnp.bfloat16).reshape(block_rows, head_cols), log_total)

    context, log_total = lax.map(
        one_block,
        (
            query_heads.reshape(block_count, block_rows, head_count, HD),
            segment.reshape(block_count, block_rows),
        ),
    )
    return (context.reshape(length, head_cols), log_total)


def attend_backward(query_heads, key_flat, value_flat, segment, grad_context, log_total):
    length, head_cols = query_heads.shape
    head_count = head_cols // HD
    block_rows = min(512, length)
    block_count = length // block_rows
    score_scale = 1.0 / math.sqrt(HD)
    key_heads = key_flat.reshape(length, head_count, HD)
    value_heads = value_flat.reshape(length, head_count, HD)

    def one_block(totals, pieces):
        grad_keys, grad_values = totals
        query_block, seg_block, grad_block, total_block = pieces
        scores = score_block(query_block, key_heads, seg_block, segment)
        prob_full = jnp.exp(scores - total_block)
        probs_low = prob_full.astype(jnp.bfloat16)
        grad_values = grad_values + jnp.einsum(
            "hbk,bhd->khd", probs_low, grad_block, preferred_element_type=jnp.float32
        )
        grad_probs = jnp.einsum(
            "bhd,khd->hbk", grad_block, value_heads, preferred_element_type=jnp.float32
        )
        row_delta = jnp.sum(prob_full * grad_probs, axis=2, keepdims=True)
        grad_scores = (prob_full * (grad_probs - row_delta)).astype(jnp.bfloat16)
        grad_query = (
            jnp.einsum("hbk,khd->bhd", grad_scores, key_heads, preferred_element_type=jnp.float32)
            * score_scale
        )
        grad_keys = grad_keys + jnp.einsum(
            "hbk,bhd->khd", grad_scores, query_block, preferred_element_type=jnp.float32
        )
        return (
            (grad_keys, grad_values),
            grad_query.astype(jnp.bfloat16).reshape(block_rows, head_cols),
        )

    empty_sum = jnp.zeros((length, head_count, HD), jnp.float32)
    (grad_keys, grad_values), grad_query = lax.scan(
        one_block,
        (empty_sum, empty_sum),
        (
            query_heads.reshape(block_count, block_rows, head_count, HD),
            segment.reshape(block_count, block_rows),
            grad_context.reshape(block_count, block_rows, head_count, HD),
            log_total,
        ),
    )
    grad_keys = (grad_keys * score_scale).astype(jnp.bfloat16).reshape(length, head_cols)
    grad_values = grad_values.astype(jnp.bfloat16).reshape(length, head_cols)
    return (grad_query.reshape(length, head_cols), grad_keys, grad_values)


def seq_gathered_grad(left, right):
    left_all = lax.all_gather(left, "seq", axis=0, tiled=True)
    right_cols = lax.all_to_all(right, "seq", split_axis=1, concat_axis=0, tiled=True)
    partial = contract_rows(left_all, right_cols).astype(jnp.bfloat16)
    summed = lax.psum_scatter(partial, "batch", scatter_dimension=0, tiled=True)
    return summed.astype(jnp.float32)


def batch_gathered_grad(left, right):
    left_rows = lax.all_to_all(left, "batch", split_axis=1, concat_axis=0, tiled=True)
    right_all = lax.all_gather(right, "batch", axis=0, tiled=True)
    partial = contract_rows(left_rows, right_all).astype(jnp.bfloat16)
    summed = lax.psum_scatter(partial, "seq", scatter_dimension=1, tiled=True)
    return summed.astype(jnp.float32)


def qkv_grad_from_heads(left, grad_heads):
    seq_count = lax.axis_size("seq")
    me = lax.axis_index("seq")
    piece = grad_heads.shape[1] // 3
    left_all = lax.all_gather(left, "seq", axis=0, tiled=True)
    partial = contract_rows(left_all, grad_heads).astype(jnp.bfloat16)
    summed = lax.psum_scatter(partial, "batch", scatter_dimension=0, tiled=True)
    summed = summed.astype(jnp.float32)
    inverse = pow(3, -1, seq_count)
    slots = []
    for slot in range(3):
        target = ((me - slot) * inverse) % seq_count
        chunk = (3 * target + slot) // seq_count
        sent = lax.dynamic_slice_in_dim(summed, chunk * piece, piece, axis=1)
        pairs = []
        for source in range(seq_count):
            pairs.append((source, ((source - slot) * inverse) % seq_count))
        slots.append(lax.ppermute(sent, "seq", pairs))
    return jnp.concatenate(slots, axis=1)


GRAD_PLAN = {"skip": "batch", "qkv": "seq", "out": "batch", "hidden": "seq", "down": "batch"}


def weight_grad(name, left, right):
    if GRAD_PLAN[name] == "seq":
        return seq_gathered_grad(left, right)
    return batch_gathered_grad(left, right)


def block(
    tokens,
    long_skip,
    lengths,
    skip_weight,
    skip_bias,
    attention_gain,
    attention_shift,
    qkv_weight,
    out_weight,
    out_bias,
    mlp_gain,
    mlp_shift,
    hidden_weight,
    hidden_bias,
    down_weight,
    down_bias,
    cotangent,
):
    local_rows = tokens.shape[1]
    feature_count = tokens.shape[2]
    group_len = local_rows * lax.axis_size("seq")
    joined = jnp.concatenate([tokens[0], long_skip[0]], axis=1)
    mixed = product(joined, skip_weight) + skip_bias.astype(jnp.float32)
    normed_full, first_pull = jax.vjp(
        layer_norm, mixed, attention_gain.astype(jnp.float32), attention_shift.astype(jnp.float32)
    )
    normed_one = normed_full.astype(jnp.bfloat16)
    packed = product(normed_one, qkv_weight).astype(jnp.bfloat16)
    seq_count = lax.axis_size("seq")
    packed_heads = lax.all_to_all(
        packed.reshape(local_rows, 3, seq_count, feature_count // seq_count),
        "seq",
        split_axis=2,
        concat_axis=0,
        tiled=True,
    ).reshape(group_len, 3, feature_count // seq_count)
    query_heads = packed_heads[:, 0]
    key_heads = packed_heads[:, 1]
    value_heads = packed_heads[:, 2]
    segment = segments(lengths[0], group_len)
    context_heads, log_total = attend_forward(query_heads, key_heads, value_heads, segment)
    context_tok = lax.all_to_all(context_heads, "seq", split_axis=0, concat_axis=1, tiled=True)
    middle = mixed + product(context_tok, out_weight) + out_bias.astype(jnp.float32)
    second_full, second_pull = jax.vjp(
        layer_norm, middle, mlp_gain.astype(jnp.float32), mlp_shift.astype(jnp.float32)
    )
    normed_two = second_full.astype(jnp.bfloat16)
    hidden_pre = product(normed_two, hidden_weight) + hidden_bias.astype(jnp.float32)
    act_full, gelu_pull = jax.vjp(exact_gelu, hidden_pre)
    hidden_act = act_full.astype(jnp.bfloat16)
    output = (middle + product(hidden_act, down_weight) + down_bias.astype(jnp.float32)).astype(
        jnp.bfloat16
    )
    grad_out_rows = cotangent[0]
    grad_down_weight = weight_grad("down", hidden_act, grad_out_rows)
    grad_down_bias = column_sums(grad_out_rows)
    grad_act = times_transposed(grad_out_rows, down_weight)
    grad_pre = gelu_pull(grad_act)[0].astype(jnp.bfloat16)
    grad_hidden_weight = weight_grad("hidden", normed_two, grad_pre)
    grad_hidden_bias = column_sums(grad_pre)
    grad_normed_two = times_transposed(grad_pre, hidden_weight)
    grad_middle_norm, grad_mlp_gain, grad_mlp_shift = second_pull(grad_normed_two)
    grad_middle = grad_out_rows.astype(jnp.float32) + grad_middle_norm
    grad_attended = grad_middle.astype(jnp.bfloat16)
    grad_out_bias = column_sums(grad_attended)
    grad_out_weight = weight_grad("out", context_tok, grad_attended)
    grad_context = times_transposed(grad_attended, out_weight).astype(jnp.bfloat16)
    grad_context_heads = lax.all_to_all(
        grad_context, "seq", split_axis=1, concat_axis=0, tiled=True
    )
    grad_query, grad_key, grad_value = attend_backward(
        query_heads, key_heads, value_heads, segment, grad_context_heads, log_total
    )
    grad_packed = jnp.concatenate(
        [
            lax.all_to_all(grad_query, "seq", split_axis=0, concat_axis=1, tiled=True),
            lax.all_to_all(grad_key, "seq", split_axis=0, concat_axis=1, tiled=True),
            lax.all_to_all(grad_value, "seq", split_axis=0, concat_axis=1, tiled=True),
        ],
        axis=1,
    )
    grad_qkv_weight = qkv_grad_from_heads(
        normed_one, jnp.concatenate([grad_query, grad_key, grad_value], axis=1)
    )
    grad_normed_one = times_transposed(grad_packed, qkv_weight)
    grad_mixed_norm, grad_attention_gain, grad_attention_shift = first_pull(grad_normed_one)
    grad_mixed = (grad_middle + grad_mixed_norm).astype(jnp.bfloat16)
    grad_skip_bias = column_sums(grad_mixed)
    grad_skip_weight = weight_grad("skip", joined, grad_mixed)
    grad_joined = times_transposed(grad_mixed, skip_weight)
    grad_tokens = grad_joined[:, :feature_count][None]
    grad_long_skip = grad_joined[:, feature_count:][None]
    summed_weights = (grad_skip_weight, grad_qkv_weight, grad_out_weight, grad_hidden_weight, grad_down_weight)
    small_grads = (
        grad_skip_bias,
        grad_attention_gain,
        grad_attention_shift,
        grad_out_bias,
        grad_mlp_gain,
        grad_mlp_shift,
        grad_hidden_bias,
        grad_down_bias,
    )
    small_sizes = [piece.shape[0] for piece in small_grads]
    small_total = lax.psum(lax.psum(jnp.concatenate(small_grads), "seq"), "batch")
    summed_small = []
    offset = 0
    for size in small_sizes:
        summed_small.append(small_total[offset : offset + size])
        offset += size
    return (
        output[None],
        grad_tokens,
        grad_long_skip,
        summed_weights[0],
        summed_small[0],
        summed_small[1],
        summed_small[2],
        summed_weights[1],
        summed_weights[2],
        summed_small[3],
        summed_small[4],
        summed_small[5],
        summed_weights[3],
        summed_small[6],
        summed_weights[4],
        summed_small[7],
    )


def solution(mesh):
    in_specs = (
        P("batch", "seq", None),
        P("batch", "seq", None),
        P("batch", None),
        P(),
        P(),
        P(),
        P(),
        P(),
        P(),
        P(),
        P(),
        P(),
        P(),
        P(),
        P(),
        P(),
        P("batch", "seq", None),
    )
    out_specs = (
        P("batch", "seq", None),
        P("batch", "seq", None),
        P("batch", "seq", None),
        P("batch", "seq"),
        P(),
        P(),
        P(),
        P("batch", "seq"),
        P("batch", "seq"),
        P(),
        P(),
        P(),
        P("batch", "seq"),
        P(),
        P("batch", "seq"),
        P(),
    )
    return jax.shard_map(block, mesh=mesh, in_specs=in_specs, out_specs=out_specs, check_vma=False)
```

```python
import math

import jax
import jax.numpy as jnp
from jax import lax
from jax.sharding import PartitionSpec as P


HD = 72


norm_eps = 1e-05


def product(left, right):
    return jnp.dot(left, right, preferred_element_type=jnp.float32)


def contract_rows(left, right):
    return lax.dot_general(
        left, right, (((0,), (0,)), ((), ())), preferred_element_type=jnp.float32
    )


def times_transposed(left, right):
    return lax.dot_general(
        left, right, (((1,), (1,)), ((), ())), preferred_element_type=jnp.float32
    )


def column_sums(values):
    return jnp.sum(values.astype(jnp.float32), axis=0)


def layer_norm(inputs, gain, shift):
    mean_row = jnp.mean(inputs, axis=-1, keepdims=True)
    centred = inputs - mean_row
    spread = jnp.mean(centred * centred, axis=-1, keepdims=True)
    return centred * lax.rsqrt(spread + norm_eps) * gain + shift


def exact_gelu(inputs):
    return jax.nn.gelu(inputs, approximate=False)


def segments(row_lengths, group_len):
    ends = jnp.cumsum(row_lengths)
    places = jnp.arange(group_len, dtype=jnp.int32)
    return jnp.sum((places[:, None] >= ends[None, :]).astype(jnp.int32), axis=1)


def score_block(query_block, key_heads, seg_block, segment):
    raw = jnp.einsum("bhd,khd->hbk", query_block, key_heads, preferred_element_type=jnp.float32)
    scores = raw * (1.0 / math.sqrt(HD))
    allowed = (seg_block[:, None] == segment[None, :])[None]
    return jnp.where(allowed, scores, -jnp.inf)


def attend_forward(query_heads, key_flat, value_flat, segment):
    length, head_cols = query_heads.shape
    head_count = head_cols // HD
    block_rows = min(512, length)
    block_count = length // block_rows
    key_heads = key_flat.reshape(length, head_count, HD)
    value_heads = value_flat.reshape(length, head_count, HD)

    def one_block(pieces):
        query_block, seg_block = pieces
        scores = score_block(query_block, key_heads, seg_block, segment)
        row_max = jnp.max(scores, axis=2, keepdims=True)
        log_total = row_max + jnp.log(jnp.sum(jnp.exp(scores - row_max), axis=2, keepdims=True))
        probs_low = jnp.exp(scores - log_total).astype(jnp.bfloat16)
        context = jnp.einsum(
            "hbk,khd->bhd", probs_low, value_heads, preferred_element_type=jnp.float32
        )
        return (context.astype(jnp.bfloat16).reshape(block_rows, head_cols), log_total)

    context, log_total = lax.map(
        one_block,
        (
            query_heads.reshape(block_count, block_rows, head_count, HD),
            segment.reshape(block_count, block_rows),
        ),
    )
    return (context.reshape(length, head_cols), log_total)


def attend_backward(query_heads, key_flat, value_flat, segment, grad_context, log_total):
    length, head_cols = query_heads.shape
    head_count = head_cols // HD
    block_rows = min(512, length)
    block_count = length // block_rows
    score_scale = 1.0 / math.sqrt(HD)
    key_heads = key_flat.reshape(length, head_count, HD)
    value_heads = value_flat.reshape(length, head_count, HD)

    def one_block(totals, pieces):
        grad_keys, grad_values = totals
        query_block, seg_block, grad_block, total_block = pieces
        scores = score_block(query_block, key_heads, seg_block, segment)
        prob_full = jnp.exp(scores - total_block)
        probs_low = prob_full.astype(jnp.bfloat16)
        grad_values = grad_values + jnp.einsum(
            "hbk,bhd->khd", probs_low, grad_block, preferred_element_type=jnp.float32
        )
        grad_probs = jnp.einsum(
            "bhd,khd->hbk", grad_block, value_heads, preferred_element_type=jnp.float32
        )
        row_delta = jnp.sum(prob_full * grad_probs, axis=2, keepdims=True)
        grad_scores = (prob_full * (grad_probs - row_delta)).astype(jnp.bfloat16)
        grad_query = (
            jnp.einsum("hbk,khd->bhd", grad_scores, key_heads, preferred_element_type=jnp.float32)
            * score_scale
        )
        grad_keys = grad_keys + jnp.einsum(
            "hbk,bhd->khd", grad_scores, query_block, preferred_element_type=jnp.float32
        )
        return (
            (grad_keys, grad_values),
            grad_query.astype(jnp.bfloat16).reshape(block_rows, head_cols),
        )

    empty_sum = jnp.zeros((length, head_count, HD), jnp.float32)
    (grad_keys, grad_values), grad_query = lax.scan(
        one_block,
        (empty_sum, empty_sum),
        (
            query_heads.reshape(block_count, block_rows, head_count, HD),
            segment.reshape(block_count, block_rows),
            grad_context.reshape(block_count, block_rows, head_count, HD),
            log_total,
        ),
    )
    grad_keys = (grad_keys * score_scale).astype(jnp.bfloat16).reshape(length, head_cols)
    grad_values = grad_values.astype(jnp.bfloat16).reshape(length, head_cols)
    return (grad_query.reshape(length, head_cols), grad_keys, grad_values)


def scatter_sum(partial, axis, dim):
    count = lax.axis_size(axis)
    shape = partial.shape
    pieces = partial.reshape(shape[:dim] + (count, shape[dim] // count) + shape[dim + 1 :])
    swapped = lax.all_to_all(pieces, axis, split_axis=dim, concat_axis=dim, tiled=True)
    return jnp.sum(swapped.astype(jnp.float32), axis=dim)


def gather_by_exchange(values, axis):
    count = lax.axis_size(axis)
    copies = jnp.broadcast_to(values[None], (count,) + values.shape)
    swapped = lax.all_to_all(copies, axis, split_axis=0, concat_axis=0, tiled=True)
    return swapped.reshape((count * values.shape[0],) + values.shape[1:])


EXCHANGE_ONLY = ("skip",)


def seq_gathered_grad(left, right):
    left_all = lax.all_gather(left, "seq", axis=0, tiled=True)
    right_cols = lax.all_to_all(right, "seq", split_axis=1, concat_axis=0, tiled=True)
    partial = contract_rows(left_all, right_cols).astype(jnp.bfloat16)
    summed = lax.psum_scatter(partial, "batch", scatter_dimension=0, tiled=True)
    return summed.astype(jnp.float32)


def batch_gathered_grad(left, right, by_exchange=False):
    left_rows = lax.all_to_all(left, "batch", split_axis=1, concat_axis=0, tiled=True)
    if by_exchange:
        right_all = gather_by_exchange(right, "batch")
    else:
        right_all = lax.all_gather(right, "batch", axis=0, tiled=True)
    partial = contract_rows(left_rows, right_all).astype(jnp.bfloat16)
    if by_exchange:
        return scatter_sum(partial, "seq", 1)
    summed = lax.psum_scatter(partial, "seq", scatter_dimension=1, tiled=True)
    return summed.astype(jnp.float32)


def qkv_grad_from_heads(left, grad_heads):
    seq_count = lax.axis_size("seq")
    me = lax.axis_index("seq")
    piece = grad_heads.shape[1] // 3
    left_all = lax.all_gather(left, "seq", axis=0, tiled=True)
    partial = contract_rows(left_all, grad_heads).astype(jnp.bfloat16)
    summed = lax.psum_scatter(partial, "batch", scatter_dimension=0, tiled=True)
    summed = summed.astype(jnp.float32)
    inverse = pow(3, -1, seq_count)
    slots = []
    for slot in range(3):
        target = ((me - slot) * inverse) % seq_count
        chunk = (3 * target + slot) // seq_count
        sent = lax.dynamic_slice_in_dim(summed, chunk * piece, piece, axis=1)
        pairs = []
        for source in range(seq_count):
            pairs.append((source, ((source - slot) * inverse) % seq_count))
        slots.append(lax.ppermute(sent, "seq", pairs))
    return jnp.concatenate(slots, axis=1)


def padded_size(sizes):
    return -(-sum(sizes) // 4096) * 4096


GRAD_PLAN = {"skip": "batch", "qkv": "seq", "out": "batch", "hidden": "seq", "down": "batch"}


def weight_grad(name, left, right):
    if GRAD_PLAN[name] == "seq":
        return seq_gathered_grad(left, right)
    return batch_gathered_grad(left, right, name in EXCHANGE_ONLY)


def block(
    tokens,
    long_skip,
    lengths,
    skip_weight,
    skip_bias,
    attention_gain,
    attention_shift,
    qkv_weight,
    out_weight,
    out_bias,
    mlp_gain,
    mlp_shift,
    hidden_weight,
    hidden_bias,
    down_weight,
    down_bias,
    cotangent,
):
    local_rows = tokens.shape[1]
    feature_count = tokens.shape[2]
    group_len = local_rows * lax.axis_size("seq")
    joined = jnp.concatenate([tokens[0], long_skip[0]], axis=1)
    mixed = product(joined, skip_weight) + skip_bias.astype(jnp.float32)
    normed_full, first_pull = jax.vjp(
        layer_norm, mixed, attention_gain.astype(jnp.float32), attention_shift.astype(jnp.float32)
    )
    normed_one = normed_full.astype(jnp.bfloat16)
    packed = product(normed_one, qkv_weight).astype(jnp.bfloat16)
    seq_count = lax.axis_size("seq")
    packed_heads = lax.all_to_all(
        packed.reshape(local_rows, 3, seq_count, feature_count // seq_count),
        "seq",
        split_axis=2,
        concat_axis=0,
        tiled=True,
    ).reshape(group_len, 3, feature_count // seq_count)
    query_heads = packed_heads[:, 0]
    key_heads = packed_heads[:, 1]
    value_heads = packed_heads[:, 2]
    segment = segments(lengths[0], group_len)
    context_heads, log_total = attend_forward(query_heads, key_heads, value_heads, segment)
    context_tok = lax.all_to_all(context_heads, "seq", split_axis=0, concat_axis=1, tiled=True)
    middle = mixed + product(context_tok, out_weight) + out_bias.astype(jnp.float32)
    second_full, second_pull = jax.vjp(
        layer_norm, middle, mlp_gain.astype(jnp.float32), mlp_shift.astype(jnp.float32)
    )
    normed_two = second_full.astype(jnp.bfloat16)
    hidden_pre = product(normed_two, hidden_weight) + hidden_bias.astype(jnp.float32)
    act_full, gelu_pull = jax.vjp(exact_gelu, hidden_pre)
    hidden_act = act_full.astype(jnp.bfloat16)
    output = (middle + product(hidden_act, down_weight) + down_bias.astype(jnp.float32)).astype(
        jnp.bfloat16
    )
    grad_out_rows = cotangent[0]
    grad_down_weight = weight_grad("down", hidden_act, grad_out_rows)
    grad_down_bias = column_sums(grad_out_rows)
    grad_act = times_transposed(grad_out_rows, down_weight)
    grad_pre = gelu_pull(grad_act)[0].astype(jnp.bfloat16)
    grad_hidden_weight = weight_grad("hidden", normed_two, grad_pre)
    grad_hidden_bias = column_sums(grad_pre)
    grad_normed_two = times_transposed(grad_pre, hidden_weight)
    grad_middle_norm, grad_mlp_gain, grad_mlp_shift = second_pull(grad_normed_two)
    grad_middle = grad_out_rows.astype(jnp.float32) + grad_middle_norm
    grad_attended = grad_middle.astype(jnp.bfloat16)
    grad_out_bias = column_sums(grad_attended)
    grad_out_weight = weight_grad("out", context_tok, grad_attended)
    grad_context = times_transposed(grad_attended, out_weight).astype(jnp.bfloat16)
    grad_context_heads = lax.all_to_all(
        grad_context, "seq", split_axis=1, concat_axis=0, tiled=True
    )
    grad_query, grad_key, grad_value = attend_backward(
        query_heads, key_heads, value_heads, segment, grad_context_heads, log_total
    )
    grad_packed = jnp.concatenate(
        [
            lax.all_to_all(grad_query, "seq", split_axis=0, concat_axis=1, tiled=True),
            lax.all_to_all(grad_key, "seq", split_axis=0, concat_axis=1, tiled=True),
            lax.all_to_all(grad_value, "seq", split_axis=0, concat_axis=1, tiled=True),
        ],
        axis=1,
    )
    grad_qkv_weight = qkv_grad_from_heads(
        normed_one, jnp.concatenate([grad_query, grad_key, grad_value], axis=1)
    )
    grad_normed_one = times_transposed(grad_packed, qkv_weight)
    grad_mixed_norm, grad_attention_gain, grad_attention_shift = first_pull(grad_normed_one)
    grad_mixed = (grad_middle + grad_mixed_norm).astype(jnp.bfloat16)
    grad_skip_bias = column_sums(grad_mixed)
    grad_skip_weight = weight_grad("skip", joined, grad_mixed)
    grad_joined = times_transposed(grad_mixed, skip_weight)
    grad_tokens = grad_joined[:, :feature_count][None]
    grad_long_skip = grad_joined[:, feature_count:][None]
    summed_weights = (grad_skip_weight, grad_qkv_weight, grad_out_weight, grad_hidden_weight, grad_down_weight)
    small_grads = (
        grad_skip_bias,
        grad_attention_gain,
        grad_attention_shift,
        grad_out_bias,
        grad_mlp_gain,
        grad_mlp_shift,
        grad_hidden_bias,
        grad_down_bias,
    )
    small_sizes = [piece.shape[0] for piece in small_grads]
    small_total = lax.psum(jnp.pad(jnp.concatenate(small_grads), (0, padded_size(small_sizes) - sum(small_sizes))), ("seq", "batch"))
    summed_small = []
    offset = 0
    for size in small_sizes:
        summed_small.append(small_total[offset : offset + size])
        offset += size
    return (
        output[None],
        grad_tokens,
        grad_long_skip,
        summed_weights[0],
        summed_small[0],
        summed_small[1],
        summed_small[2],
        summed_weights[1],
        summed_weights[2],
        summed_small[3],
        summed_small[4],
        summed_small[5],
        summed_weights[3],
        summed_small[6],
        summed_weights[4],
        summed_small[7],
    )


def solution(mesh):
    in_specs = (
        P("batch", "seq", None),
        P("batch", "seq", None),
        P("batch", None),
        P(),
        P(),
        P(),
        P(),
        P(),
        P(),
        P(),
        P(),
        P(),
        P(),
        P(),
        P(),
        P(),
        P("batch", "seq", None),
    )
    out_specs = (
        P("batch", "seq", None),
        P("batch", "seq", None),
        P("batch", "seq", None),
        P("batch", "seq"),
        P(),
        P(),
        P(),
        P("batch", "seq"),
        P("batch", "seq"),
        P(),
        P(),
        P(),
        P("batch", "seq"),
        P(),
        P("batch", "seq"),
        P(),
    )
    return jax.shard_map(block, mesh=mesh, in_specs=in_specs, out_specs=out_specs, check_vma=False)
```

```python
import math

import jax
import jax.numpy as jnp
from jax import lax
from jax.sharding import PartitionSpec as P


HD = 72


norm_eps = 1e-05


def product(left, right):
    return jnp.dot(left, right, preferred_element_type=jnp.float32)


def contract_rows(left, right):
    return lax.dot_general(
        left, right, (((0,), (0,)), ((), ())), preferred_element_type=jnp.float32
    )


def times_transposed(left, right):
    return lax.dot_general(
        left, right, (((1,), (1,)), ((), ())), preferred_element_type=jnp.float32
    )


def column_sums(values):
    return jnp.sum(values.astype(jnp.float32), axis=0)


def layer_norm(inputs, gain, shift):
    mean_row = jnp.mean(inputs, axis=-1, keepdims=True)
    centred = inputs - mean_row
    spread = jnp.mean(centred * centred, axis=-1, keepdims=True)
    return centred * lax.rsqrt(spread + norm_eps) * gain + shift


def exact_gelu(inputs):
    return jax.nn.gelu(inputs, approximate=False)


def segments(row_lengths, group_len):
    ends = jnp.cumsum(row_lengths)
    places = jnp.arange(group_len, dtype=jnp.int32)
    return jnp.sum((places[:, None] >= ends[None, :]).astype(jnp.int32), axis=1)


def score_block(query_block, key_heads, seg_block, segment):
    raw = jnp.einsum("bhd,khd->hbk", query_block, key_heads, preferred_element_type=jnp.float32)
    scores = raw * (1.0 / math.sqrt(HD))
    allowed = (seg_block[:, None] == segment[None, :])[None]
    return jnp.where(allowed, scores, -jnp.inf)


def attend_forward(query_heads, key_flat, value_flat, segment):
    length, head_cols = query_heads.shape
    head_count = head_cols // HD
    block_rows = min(512, length)
    block_count = length // block_rows
    key_heads = key_flat.reshape(length, head_count, HD)
    value_heads = value_flat.reshape(length, head_count, HD)

    def one_block(pieces):
        query_block, seg_block = pieces
        scores = score_block(query_block, key_heads, seg_block, segment)
        row_max = jnp.max(scores, axis=2, keepdims=True)
        log_total = row_max + jnp.log(jnp.sum(jnp.exp(scores - row_max), axis=2, keepdims=True))
        probs_low = jnp.exp(scores - log_total).astype(jnp.bfloat16)
        context = jnp.einsum(
            "hbk,khd->bhd", probs_low, value_heads, preferred_element_type=jnp.float32
        )
        return (context.astype(jnp.bfloat16).reshape(block_rows, head_cols), log_total)

    context, log_total = lax.map(
        one_block,
        (
            query_heads.reshape(block_count, block_rows, head_count, HD),
            segment.reshape(block_count, block_rows),
        ),
    )
    return (context.reshape(length, head_cols), log_total)


def attend_backward(query_heads, key_flat, value_flat, segment, grad_context, log_total):
    length, head_cols = query_heads.shape
    head_count = head_cols // HD
    block_rows = min(512, length)
    block_count = length // block_rows
    score_scale = 1.0 / math.sqrt(HD)
    key_heads = key_flat.reshape(length, head_count, HD)
    value_heads = value_flat.reshape(length, head_count, HD)

    def one_block(totals, pieces):
        grad_keys, grad_values = totals
        query_block, seg_block, grad_block, total_block = pieces
        scores = score_block(query_block, key_heads, seg_block, segment)
        prob_full = jnp.exp(scores - total_block)
        probs_low = prob_full.astype(jnp.bfloat16)
        grad_values = grad_values + jnp.einsum(
            "hbk,bhd->khd", probs_low, grad_block, preferred_element_type=jnp.float32
        )
        grad_probs = jnp.einsum(
            "bhd,khd->hbk", grad_block, value_heads, preferred_element_type=jnp.float32
        )
        row_delta = jnp.sum(prob_full * grad_probs, axis=2, keepdims=True)
        grad_scores = (prob_full * (grad_probs - row_delta)).astype(jnp.bfloat16)
        grad_query = (
            jnp.einsum("hbk,khd->bhd", grad_scores, key_heads, preferred_element_type=jnp.float32)
            * score_scale
        )
        grad_keys = grad_keys + jnp.einsum(
            "hbk,bhd->khd", grad_scores, query_block, preferred_element_type=jnp.float32
        )
        return (
            (grad_keys, grad_values),
            grad_query.astype(jnp.bfloat16).reshape(block_rows, head_cols),
        )

    empty_sum = jnp.zeros((length, head_count, HD), jnp.float32)
    (grad_keys, grad_values), grad_query = lax.scan(
        one_block,
        (empty_sum, empty_sum),
        (
            query_heads.reshape(block_count, block_rows, head_count, HD),
            segment.reshape(block_count, block_rows),
            grad_context.reshape(block_count, block_rows, head_count, HD),
            log_total,
        ),
    )
    grad_keys = (grad_keys * score_scale).astype(jnp.bfloat16).reshape(length, head_cols)
    grad_values = grad_values.astype(jnp.bfloat16).reshape(length, head_cols)
    return (grad_query.reshape(length, head_cols), grad_keys, grad_values)


def scatter_sum(partial, axis, dim):
    count = lax.axis_size(axis)
    shape = partial.shape
    pieces = partial.reshape(shape[:dim] + (count, shape[dim] // count) + shape[dim + 1 :])
    swapped = lax.all_to_all(pieces, axis, split_axis=dim, concat_axis=dim, tiled=True)
    return jnp.sum(swapped.astype(jnp.float32), axis=dim)


def gather_by_exchange(values, axis):
    count = lax.axis_size(axis)
    copies = jnp.broadcast_to(values[None], (count,) + values.shape)
    swapped = lax.all_to_all(copies, axis, split_axis=0, concat_axis=0, tiled=True)
    return swapped.reshape((count * values.shape[0],) + values.shape[1:])


EXCHANGE_ONLY = ("skip",)


def seq_gathered_grad(left, right):
    left_all = lax.all_gather(left, "seq", axis=0, tiled=True)
    right_cols = lax.all_to_all(right, "seq", split_axis=1, concat_axis=0, tiled=True)
    partial = contract_rows(left_all, right_cols).astype(jnp.bfloat16)
    summed = lax.psum_scatter(partial, "batch", scatter_dimension=0, tiled=True)
    return summed.astype(jnp.float32)


def batch_gathered_grad(left, right, by_exchange=False):
    left_rows = lax.all_to_all(left, "batch", split_axis=1, concat_axis=0, tiled=True)
    if by_exchange:
        right_all = gather_by_exchange(right, "batch")
    else:
        right_all = lax.all_gather(right, "batch", axis=0, tiled=True)
    partial = contract_rows(left_rows, right_all).astype(jnp.bfloat16)
    if by_exchange:
        return scatter_sum(partial, "seq", 1)
    summed = lax.psum_scatter(partial, "seq", scatter_dimension=1, tiled=True)
    return summed.astype(jnp.float32)


def qkv_grad_from_heads(left, grad_heads):
    seq_count = lax.axis_size("seq")
    me = lax.axis_index("seq")
    piece = grad_heads.shape[1] // 3
    left_all = lax.all_gather(left, "seq", axis=0, tiled=True)
    partial = contract_rows(left_all, grad_heads).astype(jnp.bfloat16)
    summed = lax.psum_scatter(partial, "batch", scatter_dimension=0, tiled=True)
    summed = summed.astype(jnp.float32)
    inverse = pow(3, -1, seq_count)
    slots = []
    for slot in range(3):
        target = ((me - slot) * inverse) % seq_count
        chunk = (3 * target + slot) // seq_count
        sent = lax.dynamic_slice_in_dim(summed, chunk * piece, piece, axis=1)
        pairs = []
        for source in range(seq_count):
            pairs.append((source, ((source - slot) * inverse) % seq_count))
        slots.append(lax.ppermute(sent, "seq", pairs))
    return jnp.concatenate(slots, axis=1)


def back_to_tokens(values):
    return lax.all_to_all(values, "seq", split_axis=0, concat_axis=1, tiled=True)


GRAD_PLAN = {"skip": "batch", "qkv": "seq", "out": "batch", "hidden": "seq", "down": "batch"}


def weight_grad(name, left, right):
    if GRAD_PLAN[name] == "seq":
        return seq_gathered_grad(left, right)
    return batch_gathered_grad(left, right, name in EXCHANGE_ONLY)


def block(
    tokens,
    long_skip,
    lengths,
    skip_weight,
    skip_bias,
    attention_gain,
    attention_shift,
    qkv_weight,
    out_weight,
    out_bias,
    mlp_gain,
    mlp_shift,
    hidden_weight,
    hidden_bias,
    down_weight,
    down_bias,
    cotangent,
):
    local_rows = tokens.shape[1]
    feature_count = tokens.shape[2]
    group_len = local_rows * lax.axis_size("seq")
    joined = jnp.concatenate([tokens[0], long_skip[0]], axis=1)
    mixed = product(joined, skip_weight) + skip_bias.astype(jnp.float32)
    normed_full, first_pull = jax.vjp(
        layer_norm, mixed, attention_gain.astype(jnp.float32), attention_shift.astype(jnp.float32)
    )
    normed_one = normed_full.astype(jnp.bfloat16)
    packed = product(normed_one, qkv_weight).astype(jnp.bfloat16)
    seq_count = lax.axis_size("seq")
    packed_heads = lax.all_to_all(
        packed.reshape(local_rows, 3, seq_count, feature_count // seq_count),
        "seq",
        split_axis=2,
        concat_axis=0,
        tiled=True,
    ).reshape(group_len, 3, feature_count // seq_count)
    query_heads = packed_heads[:, 0]
    key_heads = packed_heads[:, 1]
    value_heads = packed_heads[:, 2]
    segment = segments(lengths[0], group_len)
    context_heads, log_total = attend_forward(query_heads, key_heads, value_heads, segment)
    context_tok = lax.all_to_all(context_heads, "seq", split_axis=0, concat_axis=1, tiled=True)
    middle = mixed + product(context_tok, out_weight) + out_bias.astype(jnp.float32)
    second_full, second_pull = jax.vjp(
        layer_norm, middle, mlp_gain.astype(jnp.float32), mlp_shift.astype(jnp.float32)
    )
    normed_two = second_full.astype(jnp.bfloat16)
    hidden_pre = product(normed_two, hidden_weight) + hidden_bias.astype(jnp.float32)
    act_full, gelu_pull = jax.vjp(exact_gelu, hidden_pre)
    hidden_act = act_full.astype(jnp.bfloat16)
    output = (middle + product(hidden_act, down_weight) + down_bias.astype(jnp.float32)).astype(
        jnp.bfloat16
    )
    grad_out_rows = cotangent[0]
    grad_down_weight = weight_grad("down", hidden_act, grad_out_rows)
    grad_down_bias = column_sums(grad_out_rows)
    grad_act = times_transposed(grad_out_rows, down_weight)
    grad_pre = gelu_pull(grad_act)[0].astype(jnp.bfloat16)
    grad_hidden_weight = weight_grad("hidden", normed_two, grad_pre)
    grad_hidden_bias = column_sums(grad_pre)
    grad_normed_two = times_transposed(grad_pre, hidden_weight)
    grad_middle_norm, grad_mlp_gain, grad_mlp_shift = second_pull(grad_normed_two)
    grad_middle = grad_out_rows.astype(jnp.float32) + grad_middle_norm
    grad_attended = grad_middle.astype(jnp.bfloat16)
    grad_out_bias = column_sums(grad_attended)
    grad_out_weight = weight_grad("out", context_tok, grad_attended)
    grad_context = times_transposed(grad_attended, out_weight).astype(jnp.bfloat16)
    grad_context_heads = lax.all_to_all(
        grad_context, "seq", split_axis=1, concat_axis=0, tiled=True
    )
    grad_query, grad_key, grad_value = attend_backward(
        query_heads, key_heads, value_heads, segment, grad_context_heads, log_total
    )
    grad_packed = jnp.concatenate(
        [back_to_tokens(grad_query), back_to_tokens(grad_key), back_to_tokens(grad_value)],
        axis=1,
    )
    grad_qkv_weight = qkv_grad_from_heads(
        normed_one, jnp.concatenate([grad_query, grad_key, grad_value], axis=1)
    )
    grad_normed_one = times_transposed(grad_packed, qkv_weight)
    grad_mixed_norm, grad_attention_gain, grad_attention_shift = first_pull(grad_normed_one)
    grad_mixed = (grad_middle + grad_mixed_norm).astype(jnp.bfloat16)
    grad_skip_bias = column_sums(grad_mixed)
    grad_skip_weight = weight_grad("skip", joined, grad_mixed)
    grad_joined = times_transposed(grad_mixed, skip_weight)
    grad_tokens = grad_joined[:, :feature_count][None]
    grad_long_skip = grad_joined[:, feature_count:][None]
    summed_weights = (grad_skip_weight, grad_qkv_weight, grad_out_weight, grad_hidden_weight, grad_down_weight)
    small_grads = (
        grad_skip_bias,
        grad_attention_gain,
        grad_attention_shift,
        grad_out_bias,
        grad_mlp_gain,
        grad_mlp_shift,
        grad_hidden_bias,
        grad_down_bias,
    )
    small_sizes = [piece.shape[0] for piece in small_grads]
    small_total = lax.psum(jnp.concatenate(small_grads), ("seq", "batch"))
    summed_small = []
    offset = 0
    for size in small_sizes:
        summed_small.append(small_total[offset : offset + size])
        offset += size
    return (
        output[None],
        grad_tokens,
        grad_long_skip,
        summed_weights[0],
        summed_small[0],
        summed_small[1],
        summed_small[2],
        summed_weights[1],
        summed_weights[2],
        summed_small[3],
        summed_small[4],
        summed_small[5],
        summed_weights[3],
        summed_small[6],
        summed_weights[4],
        summed_small[7],
    )


def solution(mesh):
    in_specs = (
        P("batch", "seq", None),
        P("batch", "seq", None),
        P("batch", None),
        P(),
        P(),
        P(),
        P(),
        P(),
        P(),
        P(),
        P(),
        P(),
        P(),
        P(),
        P(),
        P(),
        P("batch", "seq", None),
    )
    out_specs = (
        P("batch", "seq", None),
        P("batch", "seq", None),
        P("batch", "seq", None),
        P("batch", "seq"),
        P(),
        P(),
        P(),
        P("batch", "seq"),
        P("batch", "seq"),
        P(),
        P(),
        P(),
        P("batch", "seq"),
        P(),
        P("batch", "seq"),
        P(),
    )
    return jax.shard_map(block, mesh=mesh, in_specs=in_specs, out_specs=out_specs, check_vma=False)
```

```python
import math

import jax
import jax.numpy as jnp
from jax import lax
from jax.sharding import PartitionSpec as P


HD = 72


norm_eps = 1e-05


def product(left, right):
    return jnp.dot(left, right, preferred_element_type=jnp.float32)


def contract_rows(left, right):
    return lax.dot_general(
        left, right, (((0,), (0,)), ((), ())), preferred_element_type=jnp.float32
    )


def times_transposed(left, right):
    return lax.dot_general(
        left, right, (((1,), (1,)), ((), ())), preferred_element_type=jnp.float32
    )


def column_sums(values):
    return jnp.sum(values.astype(jnp.float32), axis=0)


def layer_norm(inputs, gain, shift):
    mean_row = jnp.mean(inputs, axis=-1, keepdims=True)
    centred = inputs - mean_row
    spread = jnp.mean(centred * centred, axis=-1, keepdims=True)
    return centred * lax.rsqrt(spread + norm_eps) * gain + shift


def exact_gelu(inputs):
    return jax.nn.gelu(inputs, approximate=False)


def segments(row_lengths, group_len):
    ends = jnp.cumsum(row_lengths)
    places = jnp.arange(group_len, dtype=jnp.int32)
    return jnp.sum((places[:, None] >= ends[None, :]).astype(jnp.int32), axis=1)


def score_block(query_block, key_heads, seg_block, segment):
    raw = jnp.einsum("bhd,khd->hbk", query_block, key_heads, preferred_element_type=jnp.float32)
    scores = raw * (1.0 / math.sqrt(HD))
    allowed = (seg_block[:, None] == segment[None, :])[None]
    return jnp.where(allowed, scores, -jnp.inf)


def attend_forward(query_heads, key_flat, value_flat, segment):
    length, head_cols = query_heads.shape
    head_count = head_cols // HD
    block_rows = min(512, length)
    block_count = length // block_rows
    key_heads = key_flat.reshape(length, head_count, HD)
    value_heads = value_flat.reshape(length, head_count, HD)

    def one_block(pieces):
        query_block, seg_block = pieces
        scores = score_block(query_block, key_heads, seg_block, segment)
        row_max = jnp.max(scores, axis=2, keepdims=True)
        log_total = row_max + jnp.log(jnp.sum(jnp.exp(scores - row_max), axis=2, keepdims=True))
        probs_low = jnp.exp(scores - log_total).astype(jnp.bfloat16)
        context = jnp.einsum(
            "hbk,khd->bhd", probs_low, value_heads, preferred_element_type=jnp.float32
        )
        return (context.astype(jnp.bfloat16).reshape(block_rows, head_cols), log_total)

    context, log_total = lax.map(
        one_block,
        (
            query_heads.reshape(block_count, block_rows, head_count, HD),
            segment.reshape(block_count, block_rows),
        ),
    )
    return (context.reshape(length, head_cols), log_total)


def attend_backward(query_heads, key_flat, value_flat, segment, grad_context, log_total):
    length, head_cols = query_heads.shape
    head_count = head_cols // HD
    block_rows = min(512, length)
    block_count = length // block_rows
    score_scale = 1.0 / math.sqrt(HD)
    key_heads = key_flat.reshape(length, head_count, HD)
    value_heads = value_flat.reshape(length, head_count, HD)

    def one_block(totals, pieces):
        grad_keys, grad_values = totals
        query_block, seg_block, grad_block, total_block = pieces
        scores = score_block(query_block, key_heads, seg_block, segment)
        prob_full = jnp.exp(scores - total_block)
        probs_low = prob_full.astype(jnp.bfloat16)
        grad_values = grad_values + jnp.einsum(
            "hbk,bhd->khd", probs_low, grad_block, preferred_element_type=jnp.float32
        )
        grad_probs = jnp.einsum(
            "bhd,khd->hbk", grad_block, value_heads, preferred_element_type=jnp.float32
        )
        row_delta = jnp.sum(prob_full * grad_probs, axis=2, keepdims=True)
        grad_scores = (prob_full * (grad_probs - row_delta)).astype(jnp.bfloat16)
        grad_query = (
            jnp.einsum("hbk,khd->bhd", grad_scores, key_heads, preferred_element_type=jnp.float32)
            * score_scale
        )
        grad_keys = grad_keys + jnp.einsum(
            "hbk,bhd->khd", grad_scores, query_block, preferred_element_type=jnp.float32
        )
        return (
            (grad_keys, grad_values),
            grad_query.astype(jnp.bfloat16).reshape(block_rows, head_cols),
        )

    empty_sum = jnp.zeros((length, head_count, HD), jnp.float32)
    (grad_keys, grad_values), grad_query = lax.scan(
        one_block,
        (empty_sum, empty_sum),
        (
            query_heads.reshape(block_count, block_rows, head_count, HD),
            segment.reshape(block_count, block_rows),
            grad_context.reshape(block_count, block_rows, head_count, HD),
            log_total,
        ),
    )
    grad_keys = (grad_keys * score_scale).astype(jnp.bfloat16).reshape(length, head_cols)
    grad_values = grad_values.astype(jnp.bfloat16).reshape(length, head_cols)
    return (grad_query.reshape(length, head_cols), grad_keys, grad_values)


def scatter_sum(partial, axis, dim):
    count = lax.axis_size(axis)
    shape = partial.shape
    pieces = partial.reshape(shape[:dim] + (count, shape[dim] // count) + shape[dim + 1 :])
    swapped = lax.all_to_all(pieces, axis, split_axis=dim, concat_axis=dim, tiled=True)
    return jnp.sum(swapped.astype(jnp.float32), axis=dim)


def gather_by_exchange(values, axis):
    count = lax.axis_size(axis)
    copies = jnp.broadcast_to(values[None], (count,) + values.shape)
    swapped = lax.all_to_all(copies, axis, split_axis=0, concat_axis=0, tiled=True)
    return swapped.reshape((count * values.shape[0],) + values.shape[1:])


EXCHANGE_ONLY = ("skip",)


def seq_gathered_grad(left, right):
    left_all = lax.all_gather(left, "seq", axis=0, tiled=True)
    right_cols = lax.all_to_all(right, "seq", split_axis=1, concat_axis=0, tiled=True)
    partial = contract_rows(left_all, right_cols).astype(jnp.bfloat16)
    summed = lax.psum_scatter(partial, "batch", scatter_dimension=0, tiled=True)
    return summed.astype(jnp.float32)


def split_rows_together(lefts):
    count = lax.axis_size("batch")
    rows = lefts[0].shape[0]
    widths = [left.shape[1] // count for left in lefts]
    joined = jnp.concatenate(
        [left.reshape(rows, count, width) for left, width in zip(lefts, widths)], axis=2
    )
    moved = lax.all_to_all(joined, "batch", split_axis=1, concat_axis=0, tiled=True)
    moved = moved.reshape(count * rows, sum(widths))
    pieces = []
    offset = 0
    for width in widths:
        pieces.append(moved[:, offset : offset + width])
        offset += width
    return pieces


def batch_gathered_grad(left, right, by_exchange=False, left_rows=None):
    if left_rows is None:
        left_rows = lax.all_to_all(left, "batch", split_axis=1, concat_axis=0, tiled=True)
    if by_exchange:
        right_all = gather_by_exchange(right, "batch")
    else:
        right_all = lax.all_gather(right, "batch", axis=0, tiled=True)
    partial = contract_rows(left_rows, right_all).astype(jnp.bfloat16)
    if by_exchange:
        return scatter_sum(partial, "seq", 1)
    summed = lax.psum_scatter(partial, "seq", scatter_dimension=1, tiled=True)
    return summed.astype(jnp.float32)


def qkv_grad_from_heads(left, grad_heads):
    seq_count = lax.axis_size("seq")
    me = lax.axis_index("seq")
    piece = grad_heads.shape[1] // 3
    left_all = lax.all_gather(left, "seq", axis=0, tiled=True)
    partial = contract_rows(left_all, grad_heads).astype(jnp.bfloat16)
    summed = lax.psum_scatter(partial, "batch", scatter_dimension=0, tiled=True)
    summed = summed.astype(jnp.float32)
    inverse = pow(3, -1, seq_count)
    slots = []
    for slot in range(3):
        target = ((me - slot) * inverse) % seq_count
        chunk = (3 * target + slot) // seq_count
        sent = lax.dynamic_slice_in_dim(summed, chunk * piece, piece, axis=1)
        pairs = []
        for source in range(seq_count):
            pairs.append((source, ((source - slot) * inverse) % seq_count))
        slots.append(lax.ppermute(sent, "seq", pairs))
    return jnp.concatenate(slots, axis=1)


GRAD_PLAN = {"skip": "batch", "qkv": "seq", "out": "batch", "hidden": "seq", "down": "batch"}


def weight_grad(name, left, right, left_rows=None):
    if left_rows is not None:
        return batch_gathered_grad(left, right, name in EXCHANGE_ONLY, left_rows)
    if GRAD_PLAN[name] == "seq":
        return seq_gathered_grad(left, right)
    return batch_gathered_grad(left, right, name in EXCHANGE_ONLY)


def block(
    tokens,
    long_skip,
    lengths,
    skip_weight,
    skip_bias,
    attention_gain,
    attention_shift,
    qkv_weight,
    out_weight,
    out_bias,
    mlp_gain,
    mlp_shift,
    hidden_weight,
    hidden_bias,
    down_weight,
    down_bias,
    cotangent,
):
    local_rows = tokens.shape[1]
    feature_count = tokens.shape[2]
    group_len = local_rows * lax.axis_size("seq")
    joined = jnp.concatenate([tokens[0], long_skip[0]], axis=1)
    mixed = product(joined, skip_weight) + skip_bias.astype(jnp.float32)
    normed_full, first_pull = jax.vjp(
        layer_norm, mixed, attention_gain.astype(jnp.float32), attention_shift.astype(jnp.float32)
    )
    normed_one = normed_full.astype(jnp.bfloat16)
    packed = product(normed_one, qkv_weight).astype(jnp.bfloat16)
    seq_count = lax.axis_size("seq")
    packed_heads = lax.all_to_all(
        packed.reshape(local_rows, 3, seq_count, feature_count // seq_count),
        "seq",
        split_axis=2,
        concat_axis=0,
        tiled=True,
    ).reshape(group_len, 3, feature_count // seq_count)
    query_heads = packed_heads[:, 0]
    key_heads = packed_heads[:, 1]
    value_heads = packed_heads[:, 2]
    segment = segments(lengths[0], group_len)
    context_heads, log_total = attend_forward(query_heads, key_heads, value_heads, segment)
    context_tok = lax.all_to_all(context_heads, "seq", split_axis=0, concat_axis=1, tiled=True)
    middle = mixed + product(context_tok, out_weight) + out_bias.astype(jnp.float32)
    second_full, second_pull = jax.vjp(
        layer_norm, middle, mlp_gain.astype(jnp.float32), mlp_shift.astype(jnp.float32)
    )
    normed_two = second_full.astype(jnp.bfloat16)
    hidden_pre = product(normed_two, hidden_weight) + hidden_bias.astype(jnp.float32)
    act_full, gelu_pull = jax.vjp(exact_gelu, hidden_pre)
    hidden_act = act_full.astype(jnp.bfloat16)
    output = (middle + product(hidden_act, down_weight) + down_bias.astype(jnp.float32)).astype(
        jnp.bfloat16
    )
    grad_out_rows = cotangent[0]
    hidden_rows, context_rows = split_rows_together((hidden_act, context_tok))
    grad_down_weight = weight_grad("down", hidden_act, grad_out_rows, hidden_rows)
    grad_down_bias = column_sums(grad_out_rows)
    grad_act = times_transposed(grad_out_rows, down_weight)
    grad_pre = gelu_pull(grad_act)[0].astype(jnp.bfloat16)
    grad_hidden_weight = weight_grad("hidden", normed_two, grad_pre)
    grad_hidden_bias = column_sums(grad_pre)
    grad_normed_two = times_transposed(grad_pre, hidden_weight)
    grad_middle_norm, grad_mlp_gain, grad_mlp_shift = second_pull(grad_normed_two)
    grad_middle = grad_out_rows.astype(jnp.float32) + grad_middle_norm
    grad_attended = grad_middle.astype(jnp.bfloat16)
    grad_out_bias = column_sums(grad_attended)
    grad_out_weight = weight_grad("out", context_tok, grad_attended, context_rows)
    grad_context = times_transposed(grad_attended, out_weight).astype(jnp.bfloat16)
    grad_context_heads = lax.all_to_all(
        grad_context, "seq", split_axis=1, concat_axis=0, tiled=True
    )
    grad_query, grad_key, grad_value = attend_backward(
        query_heads, key_heads, value_heads, segment, grad_context_heads, log_total
    )
    grad_packed = jnp.concatenate(
        [
            lax.all_to_all(grad_query, "seq", split_axis=0, concat_axis=1, tiled=True),
            lax.all_to_all(grad_key, "seq", split_axis=0, concat_axis=1, tiled=True),
            lax.all_to_all(grad_value, "seq", split_axis=0, concat_axis=1, tiled=True),
        ],
        axis=1,
    )
    grad_qkv_weight = qkv_grad_from_heads(
        normed_one, jnp.concatenate([grad_query, grad_key, grad_value], axis=1)
    )
    grad_normed_one = times_transposed(grad_packed, qkv_weight)
    grad_mixed_norm, grad_attention_gain, grad_attention_shift = first_pull(grad_normed_one)
    grad_mixed = (grad_middle + grad_mixed_norm).astype(jnp.bfloat16)
    grad_skip_bias = column_sums(grad_mixed)
    grad_skip_weight = weight_grad("skip", joined, grad_mixed)
    grad_joined = times_transposed(grad_mixed, skip_weight)
    grad_tokens = grad_joined[:, :feature_count][None]
    grad_long_skip = grad_joined[:, feature_count:][None]
    summed_weights = (grad_skip_weight, grad_qkv_weight, grad_out_weight, grad_hidden_weight, grad_down_weight)
    small_grads = (
        grad_skip_bias,
        grad_attention_gain,
        grad_attention_shift,
        grad_out_bias,
        grad_mlp_gain,
        grad_mlp_shift,
        grad_hidden_bias,
        grad_down_bias,
    )
    small_sizes = [piece.shape[0] for piece in small_grads]
    small_total = lax.psum(jnp.concatenate(small_grads), ("seq", "batch"))
    summed_small = []
    offset = 0
    for size in small_sizes:
        summed_small.append(small_total[offset : offset + size])
        offset += size
    return (
        output[None],
        grad_tokens,
        grad_long_skip,
        summed_weights[0],
        summed_small[0],
        summed_small[1],
        summed_small[2],
        summed_weights[1],
        summed_weights[2],
        summed_small[3],
        summed_small[4],
        summed_small[5],
        summed_weights[3],
        summed_small[6],
        summed_weights[4],
        summed_small[7],
    )


def solution(mesh):
    in_specs = (
        P("batch", "seq", None),
        P("batch", "seq", None),
        P("batch", None),
        P(),
        P(),
        P(),
        P(),
        P(),
        P(),
        P(),
        P(),
        P(),
        P(),
        P(),
        P(),
        P(),
        P("batch", "seq", None),
    )
    out_specs = (
        P("batch", "seq", None),
        P("batch", "seq", None),
        P("batch", "seq", None),
        P("batch", "seq"),
        P(),
        P(),
        P(),
        P("batch", "seq"),
        P("batch", "seq"),
        P(),
        P(),
        P(),
        P("batch", "seq"),
        P(),
        P("batch", "seq"),
        P(),
    )
    return jax.shard_map(block, mesh=mesh, in_specs=in_specs, out_specs=out_specs, check_vma=False)
```

```python
import math

import jax
import jax.numpy as jnp
from jax import lax
from jax.sharding import PartitionSpec as P


HD = 72


norm_eps = 1e-05


def product(left, right):
    return jnp.dot(left, right, preferred_element_type=jnp.float32)


def contract_rows(left, right):
    return lax.dot_general(
        left, right, (((0,), (0,)), ((), ())), preferred_element_type=jnp.float32
    )


def times_transposed(left, right):
    return lax.dot_general(
        left, right, (((1,), (1,)), ((), ())), preferred_element_type=jnp.float32
    )


def column_sums(values):
    return jnp.sum(values.astype(jnp.float32), axis=0)


def layer_norm(inputs, gain, shift):
    mean_row = jnp.mean(inputs, axis=-1, keepdims=True)
    centred = inputs - mean_row
    spread = jnp.mean(centred * centred, axis=-1, keepdims=True)
    return centred * lax.rsqrt(spread + norm_eps) * gain + shift


def exact_gelu(inputs):
    return jax.nn.gelu(inputs, approximate=False)


def segments(row_lengths, group_len):
    ends = jnp.cumsum(row_lengths)
    places = jnp.arange(group_len, dtype=jnp.int32)
    return jnp.sum((places[:, None] >= ends[None, :]).astype(jnp.int32), axis=1)


def score_block(query_block, key_heads, seg_block, segment):
    raw = jnp.einsum("bhd,khd->hbk", query_block, key_heads, preferred_element_type=jnp.float32)
    scores = raw * (1.0 / math.sqrt(HD))
    allowed = (seg_block[:, None] == segment[None, :])[None]
    return jnp.where(allowed, scores, -jnp.inf)


def attend_forward(query_heads, key_flat, value_flat, segment):
    length, head_cols = query_heads.shape
    head_count = head_cols // HD
    block_rows = min(512, length)
    block_count = length // block_rows
    key_heads = key_flat.reshape(length, head_count, HD)
    value_heads = value_flat.reshape(length, head_count, HD)

    def one_block(pieces):
        query_block, seg_block = pieces
        scores = score_block(query_block, key_heads, seg_block, segment)
        row_max = jnp.max(scores, axis=2, keepdims=True)
        log_total = row_max + jnp.log(jnp.sum(jnp.exp(scores - row_max), axis=2, keepdims=True))
        probs_low = jnp.exp(scores - log_total).astype(jnp.bfloat16)
        context = jnp.einsum(
            "hbk,khd->bhd", probs_low, value_heads, preferred_element_type=jnp.float32
        )
        return (context.astype(jnp.bfloat16).reshape(block_rows, head_cols), log_total)

    context, log_total = lax.map(
        one_block,
        (
            query_heads.reshape(block_count, block_rows, head_count, HD),
            segment.reshape(block_count, block_rows),
        ),
    )
    return (context.reshape(length, head_cols), log_total)


def attend_backward(query_heads, key_flat, value_flat, segment, grad_context, log_total):
    length, head_cols = query_heads.shape
    head_count = head_cols // HD
    block_rows = min(512, length)
    block_count = length // block_rows
    score_scale = 1.0 / math.sqrt(HD)
    key_heads = key_flat.reshape(length, head_count, HD)
    value_heads = value_flat.reshape(length, head_count, HD)

    def one_block(totals, pieces):
        grad_keys, grad_values = totals
        query_block, seg_block, grad_block, total_block = pieces
        scores = score_block(query_block, key_heads, seg_block, segment)
        prob_full = jnp.exp(scores - total_block)
        probs_low = prob_full.astype(jnp.bfloat16)
        grad_values = grad_values + jnp.einsum(
            "hbk,bhd->khd", probs_low, grad_block, preferred_element_type=jnp.float32
        )
        grad_probs = jnp.einsum(
            "bhd,khd->hbk", grad_block, value_heads, preferred_element_type=jnp.float32
        )
        row_delta = jnp.sum(prob_full * grad_probs, axis=2, keepdims=True)
        grad_scores = (prob_full * (grad_probs - row_delta)).astype(jnp.bfloat16)
        grad_query = (
            jnp.einsum("hbk,khd->bhd", grad_scores, key_heads, preferred_element_type=jnp.float32)
            * score_scale
        )
        grad_keys = grad_keys + jnp.einsum(
            "hbk,bhd->khd", grad_scores, query_block, preferred_element_type=jnp.float32
        )
        return (
            (grad_keys, grad_values),
            grad_query.astype(jnp.bfloat16).reshape(block_rows, head_cols),
        )

    empty_sum = jnp.zeros((length, head_count, HD), jnp.float32)
    (grad_keys, grad_values), grad_query = lax.scan(
        one_block,
        (empty_sum, empty_sum),
        (
            query_heads.reshape(block_count, block_rows, head_count, HD),
            segment.reshape(block_count, block_rows),
            grad_context.reshape(block_count, block_rows, head_count, HD),
            log_total,
        ),
    )
    grad_keys = (grad_keys * score_scale).astype(jnp.bfloat16).reshape(length, head_cols)
    grad_values = grad_values.astype(jnp.bfloat16).reshape(length, head_cols)
    return (grad_query.reshape(length, head_cols), grad_keys, grad_values)


def scatter_sum(partial, axis, dim):
    count = lax.axis_size(axis)
    shape = partial.shape
    pieces = partial.reshape(shape[:dim] + (count, shape[dim] // count) + shape[dim + 1 :])
    swapped = lax.all_to_all(pieces, axis, split_axis=dim, concat_axis=dim, tiled=True)
    return jnp.sum(swapped.astype(jnp.float32), axis=dim)


def gather_by_exchange(values, axis):
    count = lax.axis_size(axis)
    copies = jnp.broadcast_to(values[None], (count,) + values.shape)
    swapped = lax.all_to_all(copies, axis, split_axis=0, concat_axis=0, tiled=True)
    return swapped.reshape((count * values.shape[0],) + values.shape[1:])


EXCHANGE_ONLY = ("skip",)


def seq_gathered_grad(left, right):
    left_all = lax.all_gather(left, "seq", axis=0, tiled=True)
    right_cols = lax.all_to_all(right, "seq", split_axis=1, concat_axis=0, tiled=True)
    partial = contract_rows(left_all, right_cols).astype(jnp.bfloat16)
    summed = lax.psum_scatter(partial, "batch", scatter_dimension=0, tiled=True)
    return summed.astype(jnp.float32)


def batch_gathered_grad(left, right, by_exchange=False):
    left_rows = lax.all_to_all(left, "batch", split_axis=1, concat_axis=0, tiled=True)
    if by_exchange:
        right_all = gather_by_exchange(right, "batch")
    else:
        right_all = lax.all_gather(right, "batch", axis=0, tiled=True)
    partial = contract_rows(left_rows, right_all).astype(jnp.bfloat16)
    if by_exchange:
        return scatter_sum(partial, "seq", 1)
    summed = lax.psum_scatter(partial, "seq", scatter_dimension=1, tiled=True)
    return summed.astype(jnp.float32)


def qkv_grad_from_heads(left, grad_heads):
    seq_count = lax.axis_size("seq")
    me = lax.axis_index("seq")
    piece = grad_heads.shape[1] // 3
    left_all = lax.all_gather(left, "seq", axis=0, tiled=True)
    partial = contract_rows(left_all, grad_heads).astype(jnp.bfloat16)
    inverse = pow(3, -1, seq_count)
    slots = []
    for slot in range(3):
        target = ((me - slot) * inverse) % seq_count
        chunk = (3 * target + slot) // seq_count
        sent = lax.dynamic_slice_in_dim(partial, chunk * piece, piece, axis=1)
        pairs = []
        for source in range(seq_count):
            pairs.append((source, ((source - slot) * inverse) % seq_count))
        slots.append(lax.ppermute(sent, "seq", pairs))
    placed = jnp.concatenate(slots, axis=1)
    summed = lax.psum_scatter(placed, "batch", scatter_dimension=0, tiled=True)
    return summed.astype(jnp.float32)


def split_high_low(values):
    high = values.astype(jnp.bfloat16)
    low = (values - high.astype(jnp.float32)).astype(jnp.bfloat16)
    return jnp.concatenate([high, low], axis=0)


def join_high_low(values):
    half = values.shape[0] // 2
    return values[:half] + values[half:]


def skip_grad_with_small(left, right, small):
    batch_count = lax.axis_size("batch")
    seq_count = lax.axis_size("seq")
    rows, width = right.shape
    small_rows = -(-small.shape[0] // width)
    small_flat = jnp.pad(small, (0, small_rows * width - small.shape[0]))
    left_rows = lax.all_to_all(left, "batch", split_axis=1, concat_axis=0, tiled=True)
    payload = jnp.concatenate(
        [right, split_high_low(small_flat.reshape(small_rows, width))], axis=0
    )
    got = gather_by_exchange(payload, "batch").reshape(batch_count, -1, width)
    right_all = got[:, :rows].reshape(batch_count * rows, width)
    batch_sum = join_high_low(jnp.sum(got[:, rows:].astype(jnp.float32), axis=0))
    partial = contract_rows(left_rows, right_all).astype(jnp.bfloat16)
    out_rows, cols = partial.shape
    piece = cols // seq_count
    extra = split_high_low(batch_sum).reshape(-1, 1, piece)
    extra = jnp.broadcast_to(extra, (extra.shape[0], seq_count, piece))
    pieces = jnp.concatenate([partial.reshape(out_rows, seq_count, piece), extra], axis=0)
    swapped = lax.all_to_all(pieces, "seq", split_axis=1, concat_axis=1, tiled=True)
    summed = jnp.sum(swapped.astype(jnp.float32), axis=1)
    weight_block = summed[:out_rows]
    small_sum = join_high_low(summed[out_rows:].reshape(2 * small_rows, width))
    return weight_block, small_sum.reshape(-1)[: small.shape[0]]


GRAD_PLAN = {"skip": "batch", "qkv": "seq", "out": "batch", "hidden": "seq", "down": "batch"}


def weight_grad(name, left, right):
    if GRAD_PLAN[name] == "seq":
        return seq_gathered_grad(left, right)
    return batch_gathered_grad(left, right, name in EXCHANGE_ONLY)


def block(
    tokens,
    long_skip,
    lengths,
    skip_weight,
    skip_bias,
    attention_gain,
    attention_shift,
    qkv_weight,
    out_weight,
    out_bias,
    mlp_gain,
    mlp_shift,
    hidden_weight,
    hidden_bias,
    down_weight,
    down_bias,
    cotangent,
):
    local_rows = tokens.shape[1]
    feature_count = tokens.shape[2]
    group_len = local_rows * lax.axis_size("seq")
    joined = jnp.concatenate([tokens[0], long_skip[0]], axis=1)
    mixed = product(joined, skip_weight) + skip_bias.astype(jnp.float32)
    normed_full, first_pull = jax.vjp(
        layer_norm, mixed, attention_gain.astype(jnp.float32), attention_shift.astype(jnp.float32)
    )
    normed_one = normed_full.astype(jnp.bfloat16)
    packed = product(normed_one, qkv_weight).astype(jnp.bfloat16)
    seq_count = lax.axis_size("seq")
    packed_heads = lax.all_to_all(
        packed.reshape(local_rows, 3, seq_count, feature_count // seq_count),
        "seq",
        split_axis=2,
        concat_axis=0,
        tiled=True,
    ).reshape(group_len, 3, feature_count // seq_count)
    query_heads = packed_heads[:, 0]
    key_heads = packed_heads[:, 1]
    value_heads = packed_heads[:, 2]
    segment = segments(lengths[0], group_len)
    context_heads, log_total = attend_forward(query_heads, key_heads, value_heads, segment)
    context_tok = lax.all_to_all(context_heads, "seq", split_axis=0, concat_axis=1, tiled=True)
    middle = mixed + product(context_tok, out_weight) + out_bias.astype(jnp.float32)
    second_full, second_pull = jax.vjp(
        layer_norm, middle, mlp_gain.astype(jnp.float32), mlp_shift.astype(jnp.float32)
    )
    normed_two = second_full.astype(jnp.bfloat16)
    hidden_pre = product(normed_two, hidden_weight) + hidden_bias.astype(jnp.float32)
    act_full, gelu_pull = jax.vjp(exact_gelu, hidden_pre)
    hidden_act = act_full.astype(jnp.bfloat16)
    output = (middle + product(hidden_act, down_weight) + down_bias.astype(jnp.float32)).astype(
        jnp.bfloat16
    )
    grad_out_rows = cotangent[0]
    grad_down_weight = weight_grad("down", hidden_act, grad_out_rows)
    grad_down_bias = column_sums(grad_out_rows)
    grad_act = lax.optimization_barrier(times_transposed(grad_out_rows, down_weight))
    grad_pre = gelu_pull(grad_act)[0].astype(jnp.bfloat16)
    grad_hidden_weight = weight_grad("hidden", normed_two, grad_pre)
    grad_hidden_bias = column_sums(grad_pre)
    grad_normed_two = times_transposed(grad_pre, hidden_weight)
    grad_middle_norm, grad_mlp_gain, grad_mlp_shift = second_pull(grad_normed_two)
    grad_middle = grad_out_rows.astype(jnp.float32) + grad_middle_norm
    grad_attended = grad_middle.astype(jnp.bfloat16)
    grad_out_bias = column_sums(grad_attended)
    grad_out_weight = weight_grad("out", context_tok, grad_attended)
    grad_context = times_transposed(grad_attended, out_weight).astype(jnp.bfloat16)
    grad_context_heads = lax.all_to_all(
        grad_context, "seq", split_axis=1, concat_axis=0, tiled=True
    )
    grad_query, grad_key, grad_value = attend_backward(
        query_heads, key_heads, value_heads, segment, grad_context_heads, log_total
    )
    grad_packed = jnp.concatenate(
        [
            lax.all_to_all(grad_query, "seq", split_axis=0, concat_axis=1, tiled=True),
            lax.all_to_all(grad_key, "seq", split_axis=0, concat_axis=1, tiled=True),
            lax.all_to_all(grad_value, "seq", split_axis=0, concat_axis=1, tiled=True),
        ],
        axis=1,
    )
    grad_qkv_weight = qkv_grad_from_heads(
        normed_one, jnp.concatenate([grad_query, grad_key, grad_value], axis=1)
    )
    grad_normed_one = times_transposed(grad_packed, qkv_weight)
    grad_mixed_norm, grad_attention_gain, grad_attention_shift = first_pull(grad_normed_one)
    grad_mixed = (grad_middle + grad_mixed_norm).astype(jnp.bfloat16)
    grad_skip_bias = column_sums(grad_mixed)
    grad_joined = times_transposed(grad_mixed, skip_weight)
    grad_tokens = grad_joined[:, :feature_count][None]
    grad_long_skip = grad_joined[:, feature_count:][None]
    small_grads = (
        grad_skip_bias,
        grad_attention_gain,
        grad_attention_shift,
        grad_out_bias,
        grad_mlp_gain,
        grad_mlp_shift,
        grad_hidden_bias,
        grad_down_bias,
    )
    small_sizes = [piece.shape[0] for piece in small_grads]
    grad_skip_weight, small_total = skip_grad_with_small(
        joined, grad_mixed, jnp.concatenate(small_grads)
    )
    summed_weights = (grad_skip_weight, grad_qkv_weight, grad_out_weight, grad_hidden_weight, grad_down_weight)
    summed_small = []
    offset = 0
    for size in small_sizes:
        summed_small.append(small_total[offset : offset + size])
        offset += size
    return (
        output[None],
        grad_tokens,
        grad_long_skip,
        summed_weights[0],
        summed_small[0],
        summed_small[1],
        summed_small[2],
        summed_weights[1],
        summed_weights[2],
        summed_small[3],
        summed_small[4],
        summed_small[5],
        summed_weights[3],
        summed_small[6],
        summed_weights[4],
        summed_small[7],
    )


def solution(mesh):
    in_specs = (
        P("batch", "seq", None),
        P("batch", "seq", None),
        P("batch", None),
        P(),
        P(),
        P(),
        P(),
        P(),
        P(),
        P(),
        P(),
        P(),
        P(),
        P(),
        P(),
        P(),
        P("batch", "seq", None),
    )
    out_specs = (
        P("batch", "seq", None),
        P("batch", "seq", None),
        P("batch", "seq", None),
        P("batch", "seq"),
        P(),
        P(),
        P(),
        P("batch", "seq"),
        P("batch", "seq"),
        P(),
        P(),
        P(),
        P("batch", "seq"),
        P(),
        P("batch", "seq"),
        P(),
    )
    return jax.shard_map(block, mesh=mesh, in_specs=in_specs, out_specs=out_specs, check_vma=False)
```

```python
import math

import jax
import jax.numpy as jnp
from jax import lax
from jax.sharding import PartitionSpec as P


HD = 72


norm_eps = 1e-05


def product(left, right):
    return jnp.dot(left, right, preferred_element_type=jnp.float32)


def contract_rows(left, right):
    return lax.dot_general(
        left, right, (((0,), (0,)), ((), ())), preferred_element_type=jnp.float32
    )


def times_transposed(left, right):
    return lax.dot_general(
        left, right, (((1,), (1,)), ((), ())), preferred_element_type=jnp.float32
    )


def column_sums(values):
    return jnp.sum(values.astype(jnp.float32), axis=0)


def layer_norm(inputs, gain, shift):
    mean_row = jnp.mean(inputs, axis=-1, keepdims=True)
    centred = inputs - mean_row
    spread = jnp.mean(centred * centred, axis=-1, keepdims=True)
    return centred * lax.rsqrt(spread + norm_eps) * gain + shift


def exact_gelu(inputs):
    return jax.nn.gelu(inputs, approximate=False)


def segments(row_lengths, group_len):
    ends = jnp.cumsum(row_lengths)
    places = jnp.arange(group_len, dtype=jnp.int32)
    return jnp.sum((places[:, None] >= ends[None, :]).astype(jnp.int32), axis=1)


def score_block(query_block, key_heads, seg_block, segment):
    raw = jnp.einsum("bhd,khd->hbk", query_block, key_heads, preferred_element_type=jnp.float32)
    scores = raw * (1.0 / math.sqrt(HD))
    allowed = (seg_block[:, None] == segment[None, :])[None]
    return jnp.where(allowed, scores, -jnp.inf)


def attend_forward(query_heads, key_flat, value_flat, segment):
    length, head_cols = query_heads.shape
    head_count = head_cols // HD
    block_rows = min(512, length)
    block_count = length // block_rows
    key_heads = key_flat.reshape(length, head_count, HD)
    value_heads = value_flat.reshape(length, head_count, HD)

    def one_block(pieces):
        query_block, seg_block = pieces
        scores = score_block(query_block, key_heads, seg_block, segment)
        row_max = jnp.max(scores, axis=2, keepdims=True)
        log_total = row_max + jnp.log(jnp.sum(jnp.exp(scores - row_max), axis=2, keepdims=True))
        probs_low = jnp.exp(scores - log_total).astype(jnp.bfloat16)
        context = jnp.einsum(
            "hbk,khd->bhd", probs_low, value_heads, preferred_element_type=jnp.float32
        )
        return (context.astype(jnp.bfloat16).reshape(block_rows, head_cols), log_total)

    context, log_total = lax.map(
        one_block,
        (
            query_heads.reshape(block_count, block_rows, head_count, HD),
            segment.reshape(block_count, block_rows),
        ),
    )
    return (context.reshape(length, head_cols), log_total)


def attend_backward(query_heads, key_flat, value_flat, segment, grad_context, log_total):
    length, head_cols = query_heads.shape
    head_count = head_cols // HD
    block_rows = min(512, length)
    block_count = length // block_rows
    score_scale = 1.0 / math.sqrt(HD)
    key_heads = key_flat.reshape(length, head_count, HD)
    value_heads = value_flat.reshape(length, head_count, HD)

    def one_block(totals, pieces):
        grad_keys, grad_values = totals
        query_block, seg_block, grad_block, total_block = pieces
        scores = score_block(query_block, key_heads, seg_block, segment)
        prob_full = jnp.exp(scores - total_block)
        probs_low = prob_full.astype(jnp.bfloat16)
        grad_values = grad_values + jnp.einsum(
            "hbk,bhd->khd", probs_low, grad_block, preferred_element_type=jnp.float32
        )
        grad_probs = jnp.einsum(
            "bhd,khd->hbk", grad_block, value_heads, preferred_element_type=jnp.float32
        )
        row_delta = jnp.sum(prob_full * grad_probs, axis=2, keepdims=True)
        grad_scores = (prob_full * (grad_probs - row_delta)).astype(jnp.bfloat16)
        grad_query = (
            jnp.einsum("hbk,khd->bhd", grad_scores, key_heads, preferred_element_type=jnp.float32)
            * score_scale
        )
        grad_keys = grad_keys + jnp.einsum(
            "hbk,bhd->khd", grad_scores, query_block, preferred_element_type=jnp.float32
        )
        return (
            (grad_keys, grad_values),
            grad_query.astype(jnp.bfloat16).reshape(block_rows, head_cols),
        )

    empty_sum = jnp.zeros((length, head_count, HD), jnp.float32)
    (grad_keys, grad_values), grad_query = lax.scan(
        one_block,
        (empty_sum, empty_sum),
        (
            query_heads.reshape(block_count, block_rows, head_count, HD),
            segment.reshape(block_count, block_rows),
            grad_context.reshape(block_count, block_rows, head_count, HD),
            log_total,
        ),
    )
    grad_keys = (grad_keys * score_scale).astype(jnp.bfloat16).reshape(length, head_cols)
    grad_values = grad_values.astype(jnp.bfloat16).reshape(length, head_cols)
    return (grad_query.reshape(length, head_cols), grad_keys, grad_values)


def scatter_sum(partial, axis, dim):
    count = lax.axis_size(axis)
    shape = partial.shape
    pieces = partial.reshape(shape[:dim] + (count, shape[dim] // count) + shape[dim + 1 :])
    swapped = lax.all_to_all(pieces, axis, split_axis=dim, concat_axis=dim, tiled=True)
    return jnp.sum(swapped.astype(jnp.float32), axis=dim)


def gather_by_exchange(values, axis):
    count = lax.axis_size(axis)
    copies = jnp.broadcast_to(values[None], (count,) + values.shape)
    swapped = lax.all_to_all(copies, axis, split_axis=0, concat_axis=0, tiled=True)
    return swapped.reshape((count * values.shape[0],) + values.shape[1:])


EXCHANGE_ONLY = ("skip",)


def seq_gathered_grad(left, right):
    left_all = lax.all_gather(left, "seq", axis=0, tiled=True)
    right_cols = lax.all_to_all(right, "seq", split_axis=1, concat_axis=0, tiled=True)
    partial = contract_rows(left_all, right_cols).astype(jnp.bfloat16)
    summed = lax.psum_scatter(partial, "batch", scatter_dimension=0, tiled=True)
    return summed.astype(jnp.float32)


def batch_gathered_grad(left, right, by_exchange=False):
    left_rows = lax.all_to_all(left, "batch", split_axis=1, concat_axis=0, tiled=True)
    if by_exchange:
        right_all = gather_by_exchange(right, "batch")
    else:
        right_all = lax.all_gather(right, "batch", axis=0, tiled=True)
    partial = contract_rows(left_rows, right_all).astype(jnp.bfloat16)
    if by_exchange:
        return scatter_sum(partial, "seq", 1)
    summed = lax.psum_scatter(partial, "seq", scatter_dimension=1, tiled=True)
    return summed.astype(jnp.float32)


def qkv_grad_from_heads(left, grad_heads):
    seq_count = lax.axis_size("seq")
    me = lax.axis_index("seq")
    piece = grad_heads.shape[1] // 3
    left_all = lax.all_gather(left, "seq", axis=0, tiled=True)
    partial = contract_rows(left_all, grad_heads).astype(jnp.bfloat16)
    summed = lax.psum_scatter(partial, "batch", scatter_dimension=0, tiled=True)
    summed = summed.astype(jnp.float32)
    inverse = pow(3, -1, seq_count)
    slots = []
    for slot in range(3):
        target = ((me - slot) * inverse) % seq_count
        chunk = (3 * target + slot) // seq_count
        sent = lax.dynamic_slice_in_dim(summed, chunk * piece, piece, axis=1)
        pairs = []
        for source in range(seq_count):
            pairs.append((source, ((source - slot) * inverse) % seq_count))
        slots.append(lax.ppermute(sent, "seq", pairs))
    return jnp.concatenate(slots, axis=1)


def split_high_low(values):
    high = values.astype(jnp.bfloat16)
    low = (values - high.astype(jnp.float32)).astype(jnp.bfloat16)
    return jnp.concatenate([high, low], axis=0)


def join_high_low(values):
    half = values.shape[0] // 2
    return values[:half] + values[half:]


def skip_grad_with_small(left, right, small):
    batch_count = lax.axis_size("batch")
    seq_count = lax.axis_size("seq")
    rows, width = right.shape
    small_rows = -(-small.shape[0] // width)
    small_flat = jnp.pad(small, (0, small_rows * width - small.shape[0]))
    left_rows = lax.all_to_all(left, "batch", split_axis=1, concat_axis=0, tiled=True)
    payload = jnp.concatenate(
        [right, split_high_low(small_flat.reshape(small_rows, width))], axis=0
    )
    got = gather_by_exchange(payload, "batch").reshape(batch_count, -1, width)
    right_all = got[:, :rows].reshape(batch_count * rows, width)
    batch_sum = join_high_low(jnp.sum(got[:, rows:].astype(jnp.float32), axis=0))
    partial = contract_rows(left_rows, right_all).astype(jnp.bfloat16)
    out_rows, cols = partial.shape
    piece = cols // seq_count
    extra = split_high_low(batch_sum).reshape(-1, 1, piece)
    extra = jnp.broadcast_to(extra, (extra.shape[0], seq_count, piece))
    pieces = jnp.concatenate([partial.reshape(out_rows, seq_count, piece), extra], axis=0)
    swapped = lax.all_to_all(pieces, "seq", split_axis=1, concat_axis=1, tiled=True)
    summed = jnp.sum(swapped.astype(jnp.float32), axis=1)
    weight_block = summed[:out_rows]
    small_sum = join_high_low(summed[out_rows:].reshape(2 * small_rows, width))
    return weight_block, small_sum.reshape(-1)[: small.shape[0]]


GRAD_PLAN = {"skip": "batch", "qkv": "seq", "out": "batch", "hidden": "seq", "down": "batch"}


def weight_grad(name, left, right):
    if GRAD_PLAN[name] == "seq":
        return seq_gathered_grad(left, right)
    return batch_gathered_grad(left, right, name in EXCHANGE_ONLY)


def block(
    tokens,
    long_skip,
    lengths,
    skip_weight,
    skip_bias,
    attention_gain,
    attention_shift,
    qkv_weight,
    out_weight,
    out_bias,
    mlp_gain,
    mlp_shift,
    hidden_weight,
    hidden_bias,
    down_weight,
    down_bias,
    cotangent,
):
    local_rows = tokens.shape[1]
    feature_count = tokens.shape[2]
    group_len = local_rows * lax.axis_size("seq")
    joined = jnp.concatenate([tokens[0], long_skip[0]], axis=1)
    mixed = product(joined, skip_weight) + skip_bias.astype(jnp.float32)
    normed_full, first_pull = jax.vjp(
        layer_norm, mixed, attention_gain.astype(jnp.float32), attention_shift.astype(jnp.float32)
    )
    normed_one = normed_full.astype(jnp.bfloat16)
    packed = product(normed_one, qkv_weight).astype(jnp.bfloat16)
    seq_count = lax.axis_size("seq")
    packed_heads = lax.all_to_all(
        packed.reshape(local_rows, 3, seq_count, feature_count // seq_count),
        "seq",
        split_axis=2,
        concat_axis=0,
        tiled=True,
    ).reshape(group_len, 3, feature_count // seq_count)
    query_heads = packed_heads[:, 0]
    key_heads = packed_heads[:, 1]
    value_heads = packed_heads[:, 2]
    segment = segments(lengths[0], group_len)
    context_heads, log_total = attend_forward(query_heads, key_heads, value_heads, segment)
    context_tok = lax.all_to_all(context_heads, "seq", split_axis=0, concat_axis=1, tiled=True)
    middle = mixed + product(context_tok, out_weight) + out_bias.astype(jnp.float32)
    second_full, second_pull = jax.vjp(
        layer_norm, middle, mlp_gain.astype(jnp.float32), mlp_shift.astype(jnp.float32)
    )
    normed_two = second_full.astype(jnp.bfloat16)
    hidden_pre = product(normed_two, hidden_weight) + hidden_bias.astype(jnp.float32)
    act_full, gelu_pull = jax.vjp(exact_gelu, hidden_pre)
    hidden_act = act_full.astype(jnp.bfloat16)
    output = (middle + product(hidden_act, down_weight) + down_bias.astype(jnp.float32)).astype(
        jnp.bfloat16
    )
    grad_out_rows = cotangent[0]
    grad_down_weight = weight_grad("down", hidden_act, grad_out_rows)
    grad_down_bias = column_sums(grad_out_rows)
    grad_act = lax.optimization_barrier(times_transposed(grad_out_rows, down_weight))
    grad_pre = gelu_pull(grad_act)[0].astype(jnp.bfloat16)
    grad_hidden_weight = weight_grad("hidden", normed_two, grad_pre)
    grad_hidden_bias = column_sums(grad_pre)
    grad_normed_two = times_transposed(grad_pre, hidden_weight)
    grad_middle_norm, grad_mlp_gain, grad_mlp_shift = second_pull(grad_normed_two)
    grad_middle = grad_out_rows.astype(jnp.float32) + grad_middle_norm
    grad_attended = grad_middle.astype(jnp.bfloat16)
    grad_out_bias = column_sums(grad_attended)
    grad_out_weight = weight_grad("out", context_tok, grad_attended)
    grad_context = times_transposed(grad_attended, out_weight).astype(jnp.bfloat16)
    grad_context_heads = lax.all_to_all(
        grad_context, "seq", split_axis=1, concat_axis=0, tiled=True
    )
    grad_query, grad_key, grad_value = attend_backward(
        query_heads, key_heads, value_heads, segment, grad_context_heads, log_total
    )
    grad_packed = jnp.concatenate(
        [
            lax.all_to_all(grad_query, "seq", split_axis=0, concat_axis=1, tiled=True),
            lax.all_to_all(grad_key, "seq", split_axis=0, concat_axis=1, tiled=True),
            lax.all_to_all(grad_value, "seq", split_axis=0, concat_axis=1, tiled=True),
        ],
        axis=1,
    )
    grad_qkv_weight = qkv_grad_from_heads(
        normed_one, jnp.concatenate([grad_query, grad_key, grad_value], axis=1)
    )
    grad_normed_one = times_transposed(grad_packed, qkv_weight)
    grad_mixed_norm, grad_attention_gain, grad_attention_shift = first_pull(grad_normed_one)
    grad_mixed = (grad_middle + grad_mixed_norm).astype(jnp.bfloat16)
    grad_skip_bias = column_sums(grad_mixed)
    grad_joined = times_transposed(grad_mixed, skip_weight)
    grad_tokens = grad_joined[:, :feature_count][None]
    grad_long_skip = grad_joined[:, feature_count:][None]
    small_grads = (
        grad_skip_bias,
        grad_attention_gain,
        grad_attention_shift,
        grad_out_bias,
        grad_mlp_gain,
        grad_mlp_shift,
        grad_hidden_bias,
        grad_down_bias,
    )
    small_sizes = [piece.shape[0] for piece in small_grads]
    grad_skip_weight, small_total = skip_grad_with_small(
        joined, grad_mixed, jnp.concatenate(small_grads)
    )
    summed_weights = (grad_skip_weight, grad_qkv_weight, grad_out_weight, grad_hidden_weight, grad_down_weight)
    summed_small = []
    offset = 0
    for size in small_sizes:
        summed_small.append(small_total[offset : offset + size])
        offset += size
    return (
        output[None],
        grad_tokens,
        grad_long_skip,
        summed_weights[0],
        summed_small[0],
        summed_small[1],
        summed_small[2],
        summed_weights[1],
        summed_weights[2],
        summed_small[3],
        summed_small[4],
        summed_small[5],
        summed_weights[3],
        summed_small[6],
        summed_weights[4],
        summed_small[7],
    )


def solution(mesh):
    in_specs = (
        P("batch", "seq", None),
        P("batch", "seq", None),
        P("batch", None),
        P(),
        P(),
        P(),
        P(),
        P(),
        P(),
        P(),
        P(),
        P(),
        P(),
        P(),
        P(),
        P(),
        P("batch", "seq", None),
    )
    out_specs = (
        P("batch", "seq", None),
        P("batch", "seq", None),
        P("batch", "seq", None),
        P("batch", "seq"),
        P(),
        P(),
        P(),
        P("batch", "seq"),
        P("batch", "seq"),
        P(),
        P(),
        P(),
        P("batch", "seq"),
        P(),
        P("batch", "seq"),
        P(),
    )
    return jax.shard_map(block, mesh=mesh, in_specs=in_specs, out_specs=out_specs, check_vma=False)
```
